32 devices in a mesh: seq: 8 (over z, x), head: 4 (over y, core).
Axes of the slice: x: 2, y: 2, z: 4, core: 2. Of those that a mesh axis runs over, the one named last changes fastest.
Arguments:
- tokens: bfloat16 [2048, 4608], P('seq', 'head'), may hold values from -32 to 32
- segments: int32 [2048], P('seq'), may hold values from 0 to 7, never falling along the last dimension, each value on 1 to 1024 neighbouring positions
- pre_gain: float32 [4608], replicated, may hold values from 0.1 to 1.9
- post_gain: float32 [4608], replicated, may hold values from 0.1 to 1.9
- w_query: bfloat16 [4608, 1024], P('seq', 'head'), may hold values from -0.375 to 0.375
- w_key: bfloat16 [4608, 512], P('seq', 'head'), may hold values from -0.1875 to 0.1875
- w_value: bfloat16 [4608, 512], P('seq', 'head'), may hold values from -0.09375 to 0.09375
- w_out: bfloat16 [1024, 4608], P('head', 'seq'), may hold values from -0.1875 to 0.1875
Outputs:
- mixed: bfloat16 [2048, 4608], P('seq')
The draws below stay inside these ranges and needn't reach their ends.
Inputs may be any that keep to these rules, and one draw needn't show every extreme that they name: `segments`: segment ids never fall; each of the 8 documents holds at least one token and at most 1024, one exactly 1024.
All inputs are finite; a program needn't handle non-finite values.
Results may differ from the reference program's by a relative error of at most 0.01.
Values may be sent and summed in bfloat16 or wider, within the bound.
A program may use at most 64 MiB of HBM per device.

```python
import math
import jax
import jax.numpy as jnp
import numpy as np
from jax import lax

D = 4608
HD = 128
GROUP = 2
SCALAR = 144
DOCS = 8
KV_HEADS = 4
HEADS = 8
TOKENS = 2048
MOST = 1024
N_HEAD = 4


def draw_tokens(key, part):
    first, second, third = jax.random.split(jax.random.fold_in(key, 11), 3)
    base = jnp.clip(jax.random.normal(first, (TOKENS, D), jnp.float32), -4.0, 4.0)
    rows = jnp.exp(jax.random.uniform(second, (TOKENS, 1), jnp.float32, jnp.log(0.3), jnp.log(3.0)))
    cols = jnp.exp(jax.random.uniform(third, (1, D), jnp.float32, jnp.log(0.3), jnp.log(3.0)))
    return jnp.clip(base * rows * cols, -32.0, 32.0).astype(jnp.bfloat16)


def block_scale(rng, dims, pieces, least, high):
    level, own = 1.0, jax.random.fold_in(rng, 6)
    for axis_at, blocks in pieces:
        draws = jnp.exp(jax.random.uniform(jax.random.fold_in(own, axis_at), (blocks,), jnp.float32, least / len(pieces), high / len(pieces)))
        level = level * jnp.repeat(draws, dims[axis_at] // blocks).reshape([-1 if axis == axis_at else 1 for axis in range(len(dims))])
    return level


def profile(number_of, total, reach, lean):
    loads = [(1 << 20) // math.isqrt(grade ** lean) + 1 for grade in range(2, number_of + 1)]
    spare, given = total - reach - (number_of - 1), [1] * (number_of - 1)
    while spare > 0:
        free = [i for i in range(number_of - 1) if given[i] < reach]
        whole, budget = sum([loads[i] for i in free]), spare
        for i in free:
            extra = min(reach - given[i], max(1, budget * loads[i] // whole), spare)
            given[i] = given[i] + extra
            spare = spare - extra
    return np.array([reach] + given)


def ragged(rng, number_of, total, reach, lean):
    if number_of == 2:
        one = jax.random.randint(rng, (), max(1, total - reach), min(reach, total - 1) + 1)
        return jnp.stack([one, total - one])
    tallies = jnp.asarray(profile(number_of, total, reach, lean), jnp.int32)
    couples = (number_of - 1) // 2
    giver, taker = tallies[1:1 + 2 * couples:2], tallies[2:2 + 2 * couples:2]
    margin = jnp.minimum(giver - 1, reach - taker)
    passed = jax.random.randint(jax.random.fold_in(rng, 1), (couples,), 0, 1 << 20) % (margin + 1)
    tallies = tallies.at[1:1 + 2 * couples:2].set(giver - passed).at[2:2 + 2 * couples:2].set(taker + passed)
    return tallies[jax.random.permutation(jax.random.fold_in(rng, 2), number_of)]


def centred(own_key, dims, scale, limit, shards=(), held_as=jnp.bfloat16):
    values = jax.random.normal(own_key, dims, jnp.float32) * scale
    if len(shards) > 0:
        values = block_scale(own_key, dims, shards, -0.22, 0.18) * values
    return jnp.clip(values, min=-limit, max=limit).astype(held_as)


def setup_inputs(seed: int = 0) -> dict:
    key_list = jax.random.split(jax.random.key(seed), 9)
    return {
        "tokens": draw_tokens(jax.random.fold_in(key_list[8], 71), 0),
        "segments": jnp.searchsorted(jnp.cumsum(ragged(key_list[1], DOCS, TOKENS, MOST, 2)), jnp.arange(TOKENS), side="right").astype(jnp.int32),
        "pre_gain": jnp.clip(1.0 + 0.18 * jax.random.normal(key_list[2], (D,), jnp.float32), 0.1, 1.9),
        "post_gain": jnp.clip(1.0 + 0.18 * jax.random.normal(key_list[3], (D,), jnp.float32), 0.1, 1.9),
        "w_query": centred(key_list[4], (D, HEADS * HD), (D // 16) ** -0.5, 0.375, ((0, 8), (1, 4))),
        "w_key": centred(key_list[5], (D, KV_HEADS * HD), (D // 4) ** -0.5, 0.1875, ((0, 8), (1, 4))),
        "w_value": centred(key_list[6], (D, KV_HEADS * HD), D ** -0.5, 0.09375, ((0, 8), (1, 4))),
        "w_out": centred(key_list[7], (HEADS * HD, D), (HEADS * HD) ** -0.5, 0.1875, ((0, 4), (1, 8))),
    }


EPS = 1e-06
CAP = 50.0

def rotate(values, position, width):
    count = values.shape[1] // width
    half = width // 2
    shaped = values.reshape(values.shape[0], count, width)
    freq = 10000.0 ** (-(jnp.arange(half, dtype=jnp.float32) / half))
    angle = position[:, None] * freq[None, :]
    cosine = jnp.cos(angle)[:, None, :]
    sine = jnp.sin(angle)[:, None, :]
    first = shaped[:, :, :half]
    second = shaped[:, :, half:]
    turned = jnp.concatenate([first * cosine - second * sine, second * cosine + first * sine], axis=2)
    return turned.reshape(values.shape[0], count * width)

def reference(tokens, segments, pre_gain, post_gain, w_query, w_key, w_value, w_out):
    wide = tokens.astype(jnp.float32)
    normed = (wide * lax.rsqrt(lax.optimization_barrier(jnp.mean(wide * wide, axis=1, keepdims=True)) + EPS) * pre_gain).astype(jnp.bfloat16)
    query = jnp.dot(normed, w_query, preferred_element_type=jnp.float32)
    key_proj = jnp.dot(normed, w_key, preferred_element_type=jnp.float32)
    value_proj = jnp.dot(normed, w_value, preferred_element_type=jnp.float32)
    levels = jnp.arange(DOCS, dtype=jnp.int32)
    onehot = (segments[:, None] == levels[None, :]).astype(jnp.float32)
    counts = lax.optimization_barrier(jnp.sum(onehot, axis=0))
    before = jnp.cumsum(counts) - counts
    start = lax.optimization_barrier(jnp.sum(onehot * before[None, :], axis=1))
    index_f = jnp.arange(TOKENS, dtype=jnp.int32).astype(jnp.float32)
    position = index_f - start
    heads = HEADS
    kv_count = KV_HEADS
    rq = (rotate(query, position, HD) * SCALAR ** (-0.5)).astype(jnp.bfloat16)
    rq = rq.reshape(TOKENS, heads, HD).transpose(1, 0, 2)
    rk = rotate(key_proj, position, HD).astype(jnp.bfloat16).reshape(TOKENS, kv_count, HD).transpose(1, 0, 2)
    vb = value_proj.astype(jnp.bfloat16).reshape(TOKENS, kv_count, HD).transpose(1, 0, 2)
    allowed = (index_f[None, :] >= start[:, None]) & (index_f[None, :] <= index_f[:, None])

    def head_attn(head):
        qh = rq[head]
        kh = rk[head // GROUP]
        vh = vb[head // GROUP]
        scores = jnp.dot(qh, kh.T, preferred_element_type=jnp.float32)
        capped = CAP * jnp.tanh(scores / CAP)
        weights = jnp.where(allowed, jnp.exp(capped), 0.0)
        total = jnp.dot(weights.astype(jnp.bfloat16), vh, preferred_element_type=jnp.float32)
        return (total / lax.optimization_barrier(jnp.sum(weights, axis=1))[:, None]).astype(jnp.bfloat16)
    attn = lax.map(head_attn, jnp.arange(heads, dtype=jnp.int32))
    attn = attn.transpose(1, 0, 2).reshape(TOKENS, heads * HD)
    per = heads * HD // N_HEAD
    groups = attn.reshape(TOKENS, N_HEAD, per).transpose(1, 0, 2)
    out_groups = w_out.reshape(N_HEAD, per, D)

    def add_group(total, pair):
        part = jnp.dot(pair[0], pair[1], preferred_element_type=jnp.float32).astype(jnp.bfloat16)
        part = lax.optimization_barrier(part).astype(jnp.float32)
        return (total + part, None)
    proj, unused = lax.scan(add_group, jnp.zeros((TOKENS, D), jnp.float32), (groups, out_groups))
    scale = lax.rsqrt(lax.optimization_barrier(jnp.mean(proj * proj, axis=1, keepdims=True)) + EPS)
    return (wide + proj * scale * post_gain).astype(jnp.bfloat16)
```

```python
import functools

import jax
import jax.numpy as jnp
import numpy as np
from jax import lax
from jax.experimental import pallas as pl
from jax.experimental.pallas import tpu as pltpu
from jax.sharding import PartitionSpec as P

HD = 128
GROUP = 2
SCALAR = 144
DOCS = 8


EPS = 1e-06
CAP = 50.0


def carried_in(value, axis, join, neutral):
    count, mine = (lax.axis_size(axis), lax.axis_index(axis))
    pieces = lax.all_gather(value, axis)
    subtotal = jnp.full_like(value, 0) + jnp.asarray(neutral, value.dtype)

    def step(position, subtotal):
        longer = join(subtotal, pieces[position])
        return jnp.where(position < mine, longer, subtotal)

    return lax.fori_loop(0, count - 1, step, subtotal)


def rotate(values, position, width):
    count = values.shape[1] // width
    half = width // 2
    shaped = values.reshape(values.shape[0], count, width)
    freq = 10000.0 ** (-(jnp.arange(half, dtype=jnp.float32) / half))
    angle = position[:, None] * freq[None, :]
    cosine = jnp.cos(angle)[:, None, :]
    sine = jnp.sin(angle)[:, None, :]
    first = shaped[:, :, :half]
    second = shaped[:, :, half:]
    turned = jnp.concatenate(
        [first * cosine - second * sine, second * cosine + first * sine], axis=2
    )
    return turned.reshape(values.shape[0], count * width)


def add_counts(earlier, later):
    return earlier + later


def local(tokens, segments, pre_gain, post_gain, w_query, w_key, w_value, w_out):
    rows = tokens.shape[0]
    whole = lax.all_gather(tokens, "head", axis=1, tiled=True)
    wide = whole.astype(jnp.float32)
    normed = (
        wide * lax.rsqrt(jnp.mean(wide * wide, axis=1, keepdims=True) + EPS) * pre_gain
    ).astype(jnp.bfloat16)
    pieces = (
        lax.all_gather(w_query, "seq", axis=0, tiled=True),
        lax.all_gather(w_key, "seq", axis=0, tiled=True),
        lax.all_gather(w_value, "seq", axis=0, tiled=True),
    )
    query, key_proj, value_proj = tuple(
        (jnp.dot(normed, piece, preferred_element_type=jnp.float32) for piece in pieces)
    )
    levels = jnp.arange(DOCS, dtype=jnp.int32)
    below = jnp.sum((levels[None, :] > segments[:, None]).astype(jnp.float32), axis=0)
    earlier = carried_in(below, "seq", add_counts, jnp.zeros((DOCS,), jnp.float32))
    starts = earlier + below
    onehot = (segments[:, None] == levels[None, :]).astype(jnp.float32)
    tok_start = jnp.sum(onehot * starts[None, :], axis=1)
    offset = lax.axis_index("seq") * rows
    index_f = (offset + jnp.arange(rows, dtype=jnp.int32)).astype(jnp.float32)
    position = index_f - tok_start
    kv_count = w_key.shape[1] // HD
    rq = (rotate(query, position, HD) * SCALAR ** (-0.5)).astype(jnp.bfloat16)
    rk = rotate(key_proj, position, HD).astype(jnp.bfloat16)
    vb = value_proj.astype(jnp.bfloat16)
    stacked = (
        rq.reshape(rows, kv_count, GROUP, HD)
        .transpose(1, 2, 0, 3)
        .reshape(kv_count, GROUP * rows, HD)
    )
    query_start = jnp.tile(tok_start, GROUP)
    query_index = jnp.tile(index_f, GROUP)
    empty = (
        jnp.zeros((kv_count, GROUP * rows, HD), jnp.float32),
        jnp.zeros((kv_count, GROUP * rows), jnp.float32),
    )
    keys_all = lax.all_gather(rk, "seq", axis=0, tiled=True)
    values_all = lax.all_gather(vb, "seq", axis=0, tiled=True)
    count = keys_all.shape[0]
    block = 1024
    steps_total = count // block

    def compute(offset_blk, state):
        numer, denom = state
        keys_blk = lax.dynamic_slice_in_dim(keys_all, offset_blk, block, 0).reshape(
            block, kv_count, HD
        )
        values_blk = lax.dynamic_slice_in_dim(values_all, offset_blk, block, 0).reshape(
            block, kv_count, HD
        )
        key_index = (offset_blk + jnp.arange(block, dtype=jnp.int32)).astype(jnp.float32)
        scores = jnp.einsum("cqd,kcd->cqk", stacked, keys_blk, preferred_element_type=jnp.float32)
        capped = CAP * jnp.tanh(scores / CAP)
        allowed = (key_index[None, None, :] >= query_start[None, :, None]) & (
            key_index[None, None, :] <= query_index[None, :, None]
        )
        weights = jnp.where(allowed, jnp.exp(capped), 0.0)
        numer = numer + jnp.einsum(
            "cqk,kcd->cqd",
            weights.astype(jnp.bfloat16),
            values_blk,
            preferred_element_type=jnp.float32,
        )
        denom = denom + jnp.sum(weights, axis=2)
        return (numer, denom)

    def one_block(step, state):
        offset_blk = step * block
        return compute(offset_blk, state)

    numer, denom = lax.fori_loop(0, steps_total, one_block, empty)
    attn = (numer / denom[:, :, None]).reshape(kv_count, GROUP, rows, HD).transpose(2, 0, 1, 3)
    attn = attn.reshape(rows, kv_count * GROUP * HD).astype(jnp.bfloat16)
    partial_proj = jnp.dot(
        attn, lax.all_gather(w_out, "seq", axis=1, tiled=True), preferred_element_type=jnp.float32
    )
    partial_proj = lax.optimization_barrier(partial_proj.astype(jnp.bfloat16)).astype(jnp.float32)
    summed = lax.psum(partial_proj.astype(jnp.bfloat16), "head").astype(jnp.float32)
    scale = lax.rsqrt(jnp.mean(summed * summed, axis=1, keepdims=True) + EPS)
    return (wide + summed * scale * post_gain).astype(jnp.bfloat16)


MESH = pl.DeviceIdType.MESH
BF16 = jnp.bfloat16
F32 = jnp.float32


def fits(mesh, tokens, w_key, w_out):
    seq, head = mesh.shape["seq"], mesh.shape["head"]
    width = tokens[1]
    weights = 2 * width * (w_key[1] // head) * (GROUP + 2)
    outs = 2 * w_out[0] * width
    rows = tokens[0] // seq
    rest = rows * width * (4 + 2 + 4 + 2) + tokens[0] * (w_key[1] // head) * 4
    return (
        head == 4
        and seq == 2 * head
        and w_key[1] // head == HD
        and (width // head) % 128 == 0
        and weights + outs + rest < 44 * 2**20
    )


class Line:
    def __init__(self, ref, recv, send, seq, lane, across, reach=None):
        self.ref, self.recv, self.send = ref, recv, send
        self.count = seq // 2
        self.me = lax.axis_index("seq")
        self.head = lax.axis_index("head")
        self.z = self.me // 2
        self.lane, self.side = lane, across
        self.reach = reach

    def copy(self, zz, way):
        block = 2 * zz + self.lane
        target = ((self.me + 2, self.head), (self.me - 2, self.head), self.side)[way]
        return pltpu.make_async_remote_copy(
            src_ref=self.ref(block),
            dst_ref=self.ref(block),
            send_sem=self.send.at[way, zz],
            recv_sem=self.recv.at[block],
            device_id=target,
            device_id_type=MESH,
        )

    def rises(self, zz):
        if self.reach is None:
            return (zz <= self.z) & (self.z < self.count - 1)
        return (zz <= self.z) & (self.z < self.count - 1) & (self.z - zz < self.reach)

    def sinks(self, zz):
        return (zz >= self.z) & (self.z > 0)

    def held(self, zz):
        return (zz <= self.z) & (self.z - zz <= self.reach)

    def begin(self):
        self.onward(self.z)
        self.across(self.z)

    def onward(self, zz):
        @pl.when(self.rises(zz))
        def _():
            self.copy(zz, 0).start()

        if self.reach is None:

            @pl.when(self.sinks(zz))
            def _():
                self.copy(zz, 1).start()

    def across(self, zz):
        self.copy(zz, 2).start()

    def take(self, zz):
        self.copy(zz, 2).wait_recv()

    def near(self, k):
        def act(zz):
            self.take(zz)
            self.onward(zz)
            self.across(zz)

        @pl.when(self.z >= k)
        def _():
            act(self.z - k)

        if self.reach is None:

            @pl.when(self.z + k < self.count)
            def _():
                act(self.z + k)

    def beside(self, zz):
        pltpu.make_async_remote_copy(
            src_ref=self.ref(2 * zz + 1 - self.lane),
            dst_ref=self.ref(2 * zz + 1 - self.lane),
            send_sem=self.send.at[2, zz],
            recv_sem=self.recv.at[2 * zz + 1 - self.lane],
            device_id=self.side,
            device_id_type=MESH,
        ).wait_recv()

    def pairs(self):
        for zz in range(self.count):
            if self.reach is None:
                self.beside(zz)
            else:
                pl.when(self.held(zz))(functools.partial(self.beside, zz))

    def drain(self):
        for zz in range(self.count):
            for way, told in ((0, self.rises(zz)), (1, self.sinks(zz))):
                if way == 0 or self.reach is None:
                    pl.when(told)(functools.partial(self.sent, zz, way))
            if self.reach is None:
                self.sent(zz, 2)
            else:
                pl.when(self.held(zz))(functools.partial(self.sent, zz, 2))

    def sent(self, zz, way):
        self.copy(zz, way).wait_send()


def kernel(
    seq, heads, rows, width, most,
    tok, seg_row, wq, wk, wv, wo_in, pre_in, post_in, freq_in,
    out,
    TOK, X, XN, SW, W, WO, SEG, KV, AO, ATT, PR, ACC, RQ, NUM, DEN, pre, post, freq,
    loc, x_recv, x_send, r_recv, r_send, s_recv, s_send, w_recv, w_send, w_swap,
    o_recv, o_z, o_x, o_y, o_c, k_recv, k_send, a_recv, a_send, a_core,
):
    me, head = lax.axis_index("seq"), lax.axis_index("head")
    z, x = me // 2, lax.rem(me, 2)
    y, c = head // 2, lax.rem(head, 2)
    line = seq // 2
    deep = width // seq
    cut = width // heads
    qd, kd = wq.shape[1], wk.shape[1]
    same = c == x
    other = c != x
    partner = (me, 2 * y + 1 - c)
    xn = (2 * z + 1 - x, head)
    yhead = 2 * (1 - y) + c
    yn = (me, yhead)
    rb = 2 * z + c
    hg = 2 * y + x

    def wide_block(ref, b):
        return ref.at[pl.ds(pl.multiple_of(b * deep, 16), deep)]

    def remote(src, dst, send, recv, where):
        return pltpu.make_async_remote_copy(
            src_ref=src, dst_ref=dst, send_sem=send, recv_sem=recv,
            device_id=where, device_id_type=MESH,
        )

    def o_ref(b, h):
        return WO.at[h, pl.ds(pl.multiple_of(b * deep, 16), deep)]

    l_tok = pltpu.make_async_copy(tok, TOK, loc.at[0])
    l_own = pltpu.make_async_copy(tok, X.at[0, head], loc.at[1])
    l_seg = pltpu.make_async_copy(seg_row, SEG.at[me], loc.at[2])
    l_out = pltpu.make_async_copy(wo_in, o_ref(me, head), loc.at[3])

    def w_loads(block):
        return [
            pltpu.make_async_copy(wq, block.at[:, pl.ds(0, qd)], loc.at[4]),
            pltpu.make_async_copy(wk, block.at[:, pl.ds(qd, kd)], loc.at[5]),
            pltpu.make_async_copy(wv, block.at[:, pl.ds(qd + kd, kd)], loc.at[6]),
        ]

    small = [
        pltpu.make_async_copy(pre_in, pre, loc.at[7]),
        pltpu.make_async_copy(post_in, post, loc.at[8]),
        pltpu.make_async_copy(freq_in, freq, loc.at[9]),
    ]

    @pl.when(same)
    def _():
        for move in w_loads(wide_block(W, me)):
            move.start()

    @pl.when(other)
    def _():
        for move in w_loads(SW):
            move.start()

    l_tok.start()

    @pl.when(same)
    def _():
        l_own.start()

    l_seg.start()
    l_out.start()
    for move in small:
        move.start()

    barrier = pltpu.get_barrier_semaphore()

    def greet(where):
        pl.semaphore_signal(barrier, inc=1, device_id=where, device_id_type=MESH)

    for dx in range(2):
        for dy in range(2):
            for dc in range(2):
                if dx + dy + dc > 0:
                    gx = lax.rem(x + dx, 2)
                    greet((2 * z + gx, 2 * lax.rem(y + dy, 2) + lax.rem(c + dc, 2)))

    @pl.when(z > 0)
    def _():
        greet((me - 2, head))

    @pl.when(z < line - 1)
    def _():
        greet((me + 2, head))

    ends = (z > 0).astype(jnp.int32) + (z < line - 1).astype(jnp.int32)
    pl.semaphore_wait(barrier, 7 + ends)

    segs = Line(lambda b: SEG.at[b], s_recv, s_send, seq, x, xn)
    ws = Line(lambda b: wide_block(W, b), w_recv, w_send, seq, c, partner)
    kvs = Line(lambda b: KV.at[b], k_recv, k_send, seq, c, partner, most // (2 * rows))

    swap = remote(SW, wide_block(W, me), w_swap.at[0], w_recv.at[me], (2 * z + c, hg))

    def t_copy(i):
        where = (
            (me, 2 * y + x),
            (me, 2 * (1 - y) + x),
            (2 * z + 1 - x, 2 * y + x),
            (2 * z + 1 - x, 2 * (1 - y) + x),
        )[i]
        return remote(TOK, X.at[0, head], x_send.at[i], x_recv.at[head], where)

    def o_copy(way, zz, rel):
        fx, fy = rel
        b = 2 * zz + (1 - x if fx else x)
        h = yhead if fy else head
        send, where = {
            "up": (o_z.at[0, zz], (me + 2, head)),
            "down": (o_z.at[1, zz], (me - 2, head)),
            "x": (o_x.at[fy, zz], xn),
            "y": (o_y.at[fx, zz], yn),
            "c": (o_c.at[2 * fx + fy, zz], partner),
        }[way]
        return remote(o_ref(b, h), o_ref(b, h), send, o_recv.at[b, h], where)

    def o_z_onward(zz):
        @pl.when((zz <= z) & (z < line - 1))
        def _():
            o_copy("up", zz, (0, 0)).start()

        @pl.when((zz >= z) & (z > 0))
        def _():
            o_copy("down", zz, (0, 0)).start()

    def o_share(zz):
        o_copy("x", zz, (0, 0)).start()
        o_copy("y", zz, (0, 0)).start()
        o_copy("c", zz, (0, 0)).start()

    def o_take(zz, rel):
        o_copy("c", zz, rel).wait_recv()

    def both(k, act):
        if k == 0:
            act(z)
        else:

            @pl.when(z >= k)
            def _():
                act(z - k)

            @pl.when(z + k < line)
            def _():
                act(z + k)

    def o_from_z(zz):
        o_take(zz, (0, 0))
        o_z_onward(zz)
        o_share(zz)

    def o_from_x(zz):
        o_take(zz, (1, 0))

        @pl.when(lax.rem(zz, 2) == 1)
        def _():
            o_copy("y", zz, (1, 0)).start()

        o_copy("c", zz, (1, 0)).start()

    def o_from_y(zz):
        o_take(zz, (0, 1))

        @pl.when(lax.rem(zz, 2) == 0)
        def _():
            o_copy("x", zz, (0, 1)).start()

        o_copy("c", zz, (0, 1)).start()

    def o_from_d(zz):
        o_take(zz, (1, 1))
        o_copy("c", zz, (1, 1)).start()

    def o_from_c(zz):
        for bx in range(2):
            for hy in range(2):
                b, h = 2 * zz + bx, 2 * hy + 1 - c
                remote(o_ref(b, h), o_ref(b, h), o_c.at[0, zz], o_recv.at[b, h], partner).wait_recv()

    @pl.when(same)
    def _():
        for move in w_loads(wide_block(W, me)):
            move.wait()
        ws.begin()

    @pl.when(other)
    def _():
        for move in w_loads(SW):
            move.wait()
        swap.start()

    l_seg.wait()
    segs.begin()
    l_tok.wait()
    t_copy(1).start()

    @pl.when(other)
    def _():
        t_copy(0).start()
        t_copy(2).start()
        t_copy(3).start()
        ws.take(z)
        ws.begin()

    l_out.wait()
    o_z_onward(z)
    ws.near(1)

    @pl.when(same)
    def _():
        t_copy(2).start()
        t_copy(3).start()

    o_share(z)
    for k in range(1, line):
        segs.near(k)
    segs.pairs()
    for move in small:
        move.wait()

    own = jnp.broadcast_to(SEG[rb].astype(F32), (HD, rows))
    col = jnp.transpose(own)[:, 0:1]
    start = jnp.zeros((rows, 1), F32)
    for j in range(seq):
        start += jnp.sum((SEG[j].astype(F32) < col).astype(F32), axis=1, keepdims=True)
    index = (rb * rows + lax.broadcasted_iota(jnp.int32, (rows, 1), 0)).astype(F32)
    angle = (index - start) * freq[...]
    cosine = jnp.cos(angle)
    sine = jnp.sin(angle)
    lane = lax.broadcasted_iota(jnp.int32, (rows, HD), 1)
    sine = jnp.where(lane < HD // 2, -sine, sine)

    ws.near(2)
    both(1, o_from_z)

    def x_take(h):
        remote(TOK, X.at[0, h], x_send.at[0], x_recv.at[h], partner).wait_recv()

    def r_copy(h):
        return remote(X.at[0, h], X.at[1, h], r_send.at[h], r_recv.at[h], partner)

    for h in range(heads):
        @pl.when(same & (head == h))
        def _():
            l_own.wait()

        @pl.when(other | (head != h))
        def _():
            x_take(h)

        @pl.when(same)
        def _():
            r_copy(h).start()

    half = rows // 2

    def norm_rows(r, _):
        at = pl.ds(pl.multiple_of(r * half, half), half)
        total = jnp.zeros((half, 1), F32)
        for h in range(heads):
            wide = X[0, h, at, :].astype(F32)
            total += jnp.sum(wide * wide, axis=1, keepdims=True)
        scale = lax.rsqrt(total / width + EPS)
        for h in range(heads):
            gain = pre[h * cut : (h + 1) * cut][None, :]
            XN[h, at, :] = (X[0, h, at, :].astype(F32) * scale * gain).astype(BF16)
        return 0

    lax.fori_loop(0, 2, norm_rows, 0)
    o_from_x(z)
    o_from_y(z)
    o_from_d(z)
    for k in range(3, line):
        ws.near(k)
    ws.pairs()

    ACC[...] = jnp.zeros_like(ACC)

    def project(h, _):
        part = W[pl.ds(pl.multiple_of(h * cut, 128), cut), :]
        ACC[...] += jnp.dot(XN[h], part, preferred_element_type=F32)
        return 0

    lax.fori_loop(0, heads, project, 0)

    def turn(values):
        return values * cosine + pltpu.roll(values, HD // 2, 1) * sine

    KV[rb, :, 0:HD] = turn(ACC[:, qd : qd + HD]).astype(BF16)
    KV[rb, :, HD : 2 * HD] = ACC[:, qd + kd : qd + kd + HD].astype(BF16)
    kvs.begin()
    for g in range(GROUP):
        RQ[g * rows : (g + 1) * rows, :] = (
            turn(ACC[:, g * HD : (g + 1) * HD]) * SCALAR ** (-0.5)
        ).astype(BF16)

    both(1, o_from_x)
    both(1, o_from_y)
    both(1, o_from_d)
    kvs.near(1)
    both(2, o_from_z)
    for k in range(2, kvs.reach + 1):
        kvs.near(k)
    kvs.pairs()

    start2 = jnp.concatenate([start] * GROUP, axis=0)
    index2 = jnp.concatenate([index] * GROUP, axis=0)
    NUM[...] = jnp.zeros_like(NUM)
    DEN[...] = jnp.zeros_like(DEN)

    def attend(j, _):
        s = lax.dot_general(
            RQ[...], KV[j, :, 0:HD], (((1,), (1,)), ((), ())), preferred_element_type=F32
        )
        at = (j * rows + lax.broadcasted_iota(jnp.int32, (1, rows), 1)).astype(F32)
        p = jnp.where(
            (at >= start2) & (at <= index2), jnp.exp(CAP * jnp.tanh(s * (1.0 / CAP))), 0.0
        )
        DEN[...] += jnp.sum(p, axis=1, keepdims=True)
        NUM[...] += jnp.dot(p.astype(BF16), KV[j, :, HD : 2 * HD], preferred_element_type=F32)
        return 0

    lax.fori_loop(jnp.maximum(rb - most // rows, 0), rb + 1, attend, 0)
    ratio = (NUM[...] / DEN[:, 0:1]).astype(BF16)
    for g in range(GROUP):
        AO[:, g * HD : (g + 1) * HD] = ratio[g * rows : (g + 1) * rows, :]

    def a_copy(i):
        where = (
            (me, 2 * y + 1 - c),
            (me, yhead),
            (2 * z + 1 - x, head),
            (2 * z + 1 - x, yhead),
        )[i]
        return remote(AO, ATT.at[hg], a_send.at[i], a_recv.at[hg], where)

    def a_pass(h):
        return remote(ATT.at[h], ATT.at[h], a_core.at[h], a_recv.at[h], partner)

    @pl.when(same)
    def _():
        a_copy(1).start()
        a_copy(0).start()
        for g in range(GROUP):
            ATT[hg, :, g * HD : (g + 1) * HD] = ratio[g * rows : (g + 1) * rows, :]

    @pl.when(other)
    def _():
        a_copy(2).start()
        a_copy(3).start()

    both(2, o_from_x)
    both(2, o_from_y)
    both(2, o_from_d)
    if line > 3:
        both(3, o_from_z)

    @pl.when(same)
    def _():
        for h in (2 * (1 - y) + x, 2 * y + 1 - x, 2 * (1 - y) + 1 - x):
            a_pass(h).wait_recv()
            a_pass(h).start()

    @pl.when(other)
    def _():
        for h in range(heads):
            a_pass(h).wait_recv()

        for h in range(heads):
            r_copy(h).wait_recv()

    def emit(n):
        at = pl.ds(pl.multiple_of(n * cut, 128), cut)
        acc = jnp.zeros((rows, cut), F32)
        for h in range(heads):
            acc += lax.dot_general(
                ATT[h], WO[h, at, :], (((1,), (1,)), ((), ())), preferred_element_type=F32
            )
        PR[n] = acc
        DEN[0:rows, 0:1] += jnp.sum(acc * acc, axis=1, keepdims=True)

    DEN[...] = jnp.zeros_like(DEN)
    for k in range(line):
        if k == 3:
            both(3, o_from_x)
            both(3, o_from_y)
            both(3, o_from_d)
        both(k, o_from_c)
        both(k, emit)
    scale = lax.rsqrt(DEN[0:rows, 0:1] / width + EPS)
    kept = other.astype(jnp.int32)

    for h in range(heads):
        at = slice(h * cut, (h + 1) * cut)
        out[:, at] = (
            X[kept, h].astype(F32) + PR[h] * scale * post[at][None, :]
        ).astype(BF16)

    for stream in (segs, ws, kvs):
        stream.drain()
    t_copy(1).wait_send()
    t_copy(2).wait_send()
    t_copy(3).wait_send()

    @pl.when(other)
    def _():
        swap.wait_send()
        t_copy(0).wait_send()
        a_copy(2).wait_send()
        a_copy(3).wait_send()

    @pl.when(same)
    def _():
        a_copy(0).wait_send()
        a_copy(1).wait_send()
        for h in (2 * (1 - y) + x, 2 * y + 1 - x, 2 * (1 - y) + 1 - x):
            a_pass(h).wait_send()
        for h in range(heads):
            r_copy(h).wait_send()

    for zz in range(line):
        @pl.when((zz <= z) & (z < line - 1))
        def _():
            o_copy("up", zz, (0, 0)).wait_send()

        @pl.when((zz >= z) & (z > 0))
        def _():
            o_copy("down", zz, (0, 0)).wait_send()

        o_copy("x", zz, (0, 0)).wait_send()
        o_copy("y", zz, (0, 0)).wait_send()
        if zz % 2 == 1:
            o_copy("y", zz, (1, 0)).wait_send()
        else:
            o_copy("x", zz, (0, 1)).wait_send()
        for rel in ((0, 0), (1, 0), (0, 1), (1, 1)):
            o_copy("c", zz, rel).wait_send()


def fused(tokens, segments, pre_gain, post_gain, w_query, w_key, w_value, w_out):
    seq, heads = lax.axis_size("seq"), lax.axis_size("head")
    rows, cut = tokens.shape
    width = cut * heads
    deep = width // seq
    line = seq // 2
    qd, kd = w_query.shape[1], w_key.shape[1]
    most = rows * seq // 2
    half = HD // 2
    freq = np.float32(10000.0) ** (-(np.arange(half, dtype=np.float32) / np.float32(half)))
    freq = np.concatenate([freq, freq])[None, :].astype(np.float32)
    hbm = pl.BlockSpec(memory_space=pl.ANY)
    vmem = pl.BlockSpec(memory_space=pltpu.VMEM)
    dma = pltpu.SemaphoreType.DMA
    return pl.pallas_call(
        functools.partial(kernel, seq, heads, rows, width, most),
        out_shape=jax.ShapeDtypeStruct((rows, width), BF16),
        in_specs=[hbm] * 9,
        out_specs=vmem,
        scratch_shapes=[
            pltpu.VMEM((rows, cut), BF16),
            pltpu.VMEM((2, heads, rows, cut), BF16),
            pltpu.VMEM((heads, rows, cut), BF16),
            pltpu.VMEM((deep, qd + 2 * kd), BF16),
            pltpu.VMEM((width, qd + 2 * kd), BF16),
            pltpu.VMEM((heads, width, w_out.shape[0]), BF16),
            pltpu.VMEM((seq, 1, rows), jnp.int32),
            pltpu.VMEM((seq, rows, 2 * HD), BF16),
            pltpu.VMEM((rows, GROUP * HD), BF16),
            pltpu.VMEM((heads, rows, GROUP * HD), BF16),
            pltpu.VMEM((heads, rows, cut), F32),
            pltpu.VMEM((rows, qd + 2 * kd), F32),
            pltpu.VMEM((GROUP * rows, HD), BF16),
            pltpu.VMEM((GROUP * rows, HD), F32),
            pltpu.VMEM((GROUP * rows, HD), F32),
            pltpu.VMEM((width,), F32),
            pltpu.VMEM((width,), F32),
            pltpu.VMEM((1, HD), F32),
            dma((10,)),
            dma((heads,)), dma((4,)), dma((heads,)), dma((heads,)),
            dma((seq,)), dma((3, line)),
            dma((seq,)), dma((3, line)), dma((1,)),
            dma((seq, heads)), dma((2, line)), dma((2, line)), dma((2, line)), dma((4, line)),
            dma((seq,)), dma((3, line)),
            dma((heads,)), dma((4,)), dma((heads,)),
        ],
        compiler_params=pltpu.CompilerParams(
            collective_id=0, has_side_effects=True, vmem_limit_bytes=56 * 2**20
        ),
    )(
        tokens, segments[None, :], w_query, w_key, w_value, w_out.T,
        pre_gain, post_gain, freq,
    )


def solution(mesh):
    specs = (
        P("seq", "head"),
        P("seq"),
        P(),
        P(),
        P("seq", "head"),
        P("seq", "head"),
        P("seq", "head"),
        P("head", "seq"),
    )

    def run(*args):
        small = fits(mesh, args[0].shape, args[5].shape, args[7].shape)
        return jax.shard_map(
            fused if small else local,
            mesh=mesh,
            in_specs=specs,
            out_specs=P("seq", None),
            check_vma=False,
        )(*args)

    return run
```

```python
import enum
import functools

import jax
import jax.numpy as jnp
import numpy as np
from jax import lax
from jax.experimental import pallas as pl
from jax.experimental.pallas import tpu as pltpu
from jax.sharding import PartitionSpec as P

HD = 128
GROUP = 2
SCALAR = 144
DOCS = 8


EPS = 1e-06
CAP = 50.0


def carried_in(value, axis, join, neutral):
    count, mine = (lax.axis_size(axis), lax.axis_index(axis))
    pieces = lax.all_gather(value, axis)
    subtotal = jnp.full_like(value, 0) + jnp.asarray(neutral, value.dtype)

    def step(position, subtotal):
        longer = join(subtotal, pieces[position])
        return jnp.where(position < mine, longer, subtotal)

    return lax.fori_loop(0, count - 1, step, subtotal)


def rotate(values, position, width):
    count = values.shape[1] // width
    half = width // 2
    shaped = values.reshape(values.shape[0], count, width)
    freq = 10000.0 ** (-(jnp.arange(half, dtype=jnp.float32) / half))
    angle = position[:, None] * freq[None, :]
    cosine = jnp.cos(angle)[:, None, :]
    sine = jnp.sin(angle)[:, None, :]
    first = shaped[:, :, :half]
    second = shaped[:, :, half:]
    turned = jnp.concatenate(
        [first * cosine - second * sine, second * cosine + first * sine], axis=2
    )
    return turned.reshape(values.shape[0], count * width)


def add_counts(earlier, later):
    return earlier + later


def local(tokens, segments, pre_gain, post_gain, w_query, w_key, w_value, w_out):
    rows = tokens.shape[0]
    whole = lax.all_gather(tokens, "head", axis=1, tiled=True)
    wide = whole.astype(jnp.float32)
    normed = (
        wide * lax.rsqrt(jnp.mean(wide * wide, axis=1, keepdims=True) + EPS) * pre_gain
    ).astype(jnp.bfloat16)
    pieces = (
        lax.all_gather(w_query, "seq", axis=0, tiled=True),
        lax.all_gather(w_key, "seq", axis=0, tiled=True),
        lax.all_gather(w_value, "seq", axis=0, tiled=True),
    )
    query, key_proj, value_proj = tuple(
        (jnp.dot(normed, piece, preferred_element_type=jnp.float32) for piece in pieces)
    )
    levels = jnp.arange(DOCS, dtype=jnp.int32)
    below = jnp.sum((levels[None, :] > segments[:, None]).astype(jnp.float32), axis=0)
    earlier = carried_in(below, "seq", add_counts, jnp.zeros((DOCS,), jnp.float32))
    starts = earlier + below
    onehot = (segments[:, None] == levels[None, :]).astype(jnp.float32)
    tok_start = jnp.sum(onehot * starts[None, :], axis=1)
    offset = lax.axis_index("seq") * rows
    index_f = (offset + jnp.arange(rows, dtype=jnp.int32)).astype(jnp.float32)
    position = index_f - tok_start
    kv_count = w_key.shape[1] // HD
    rq = (rotate(query, position, HD) * SCALAR ** (-0.5)).astype(jnp.bfloat16)
    rk = rotate(key_proj, position, HD).astype(jnp.bfloat16)
    vb = value_proj.astype(jnp.bfloat16)
    stacked = (
        rq.reshape(rows, kv_count, GROUP, HD)
        .transpose(1, 2, 0, 3)
        .reshape(kv_count, GROUP * rows, HD)
    )
    query_start = jnp.tile(tok_start, GROUP)
    query_index = jnp.tile(index_f, GROUP)
    empty = (
        jnp.zeros((kv_count, GROUP * rows, HD), jnp.float32),
        jnp.zeros((kv_count, GROUP * rows), jnp.float32),
    )
    keys_all = lax.all_gather(rk, "seq", axis=0, tiled=True)
    values_all = lax.all_gather(vb, "seq", axis=0, tiled=True)
    count = keys_all.shape[0]
    block = 1024
    steps_total = count // block

    def compute(offset_blk, state):
        numer, denom = state
        keys_blk = lax.dynamic_slice_in_dim(keys_all, offset_blk, block, 0).reshape(
            block, kv_count, HD
        )
        values_blk = lax.dynamic_slice_in_dim(values_all, offset_blk, block, 0).reshape(
            block, kv_count, HD
        )
        key_index = (offset_blk + jnp.arange(block, dtype=jnp.int32)).astype(jnp.float32)
        scores = jnp.einsum("cqd,kcd->cqk", stacked, keys_blk, preferred_element_type=jnp.float32)
        capped = CAP * jnp.tanh(scores / CAP)
        allowed = (key_index[None, None, :] >= query_start[None, :, None]) & (
            key_index[None, None, :] <= query_index[None, :, None]
        )
        weights = jnp.where(allowed, jnp.exp(capped), 0.0)
        numer = numer + jnp.einsum(
            "cqk,kcd->cqd",
            weights.astype(jnp.bfloat16),
            values_blk,
            preferred_element_type=jnp.float32,
        )
        denom = denom + jnp.sum(weights, axis=2)
        return (numer, denom)

    def one_block(step, state):
        offset_blk = step * block
        return compute(offset_blk, state)

    numer, denom = lax.fori_loop(0, steps_total, one_block, empty)
    attn = (numer / denom[:, :, None]).reshape(kv_count, GROUP, rows, HD).transpose(2, 0, 1, 3)
    attn = attn.reshape(rows, kv_count * GROUP * HD).astype(jnp.bfloat16)
    partial_proj = jnp.dot(
        attn, lax.all_gather(w_out, "seq", axis=1, tiled=True), preferred_element_type=jnp.float32
    )
    partial_proj = lax.optimization_barrier(partial_proj.astype(jnp.bfloat16)).astype(jnp.float32)
    summed = lax.psum(partial_proj.astype(jnp.bfloat16), "head").astype(jnp.float32)
    scale = lax.rsqrt(jnp.mean(summed * summed, axis=1, keepdims=True) + EPS)
    return (wide + summed * scale * post_gain).astype(jnp.bfloat16)


MESH = pl.DeviceIdType.MESH
BF16 = jnp.bfloat16
F32 = jnp.float32
LINE = 4
REACH = LINE // 2
PIECES = 1
OVER_X = (0,)

class E(enum.Enum):
    K1 = enum.auto()
    K2 = enum.auto()
    Kp = enum.auto()
    Od0 = enum.auto()
    Od1 = enum.auto()
    Od2 = enum.auto()
    Od3 = enum.auto()
    On0 = enum.auto()
    On1 = enum.auto()
    On2 = enum.auto()
    On3 = enum.auto()
    Ox0 = enum.auto()
    Ox1 = enum.auto()
    Ox2 = enum.auto()
    Ox3 = enum.auto()
    Oy0 = enum.auto()
    Oy1 = enum.auto()
    Oy2 = enum.auto()
    Oy3 = enum.auto()
    Pk = enum.auto()
    Pq = enum.auto()
    Sh0 = enum.auto()
    Sh1 = enum.auto()
    Sh2 = enum.auto()
    Sh3 = enum.auto()
    Sk = enum.auto()
    Sq = enum.auto()
    TF = enum.auto()
    Tp = enum.auto()
    Tx = enum.auto()
    Ty = enum.auto()
    W0k = enum.auto()
    W0q = enum.auto()
    Wk1 = enum.auto()
    Wk2 = enum.auto()
    Wk3 = enum.auto()
    Wq1 = enum.auto()
    Wq2 = enum.auto()
    Wq3 = enum.auto()


PLAN = {
    (0, 0): (
        (E.Tp, E.W0q, E.Ty, E.On0, E.W0k,),
        (E.Sh0, E.Tx, E.On1, E.TF, E.Sh1, E.Wk1, E.Wq2, E.Oy1, E.Wk3, E.Sq, E.On2, E.Sh2, E.Sk, E.Oy0, E.Wq1, E.Wk2, E.Ox1, E.Wq3,),
        (E.Pk,),
        (E.K1, E.Ox2, E.On3, E.Ox0, E.Oy2, E.Sh3, E.Oy3, E.Pq, E.Od0, E.Od2, E.Od1,),
        (E.K2, E.Kp,),
        (),
        (E.Ox3,),
        (),
        (),
        (E.Od3,),
    ),
    (0, 1): (
        (E.Ty, E.W0k, E.On0, E.Tx, E.Sh0, E.Ox0,),
        (E.Tp, E.W0q, E.TF, E.On1, E.Sh1, E.Sk, E.On2, E.Wk2, E.Wk1, E.Sh2,),
        (E.Wk3, E.Sq, E.Wq1, E.K1, E.Pk, E.Ox1, E.Oy1, E.Oy0, E.Od0,),
        (E.K2, E.Wq2, E.Wq3, E.Ox2, E.Kp, E.Pq,),
        (E.Ox3, E.On3, E.Sh3, E.Od1,),
        (E.Od2, E.Od3, E.Oy2,),
        (),
        (E.Oy3,),
        (),
        (),
    ),
    (1, 0): (
        (E.Oy3, E.Ty, E.Tp, E.W0k, E.W0q,),
        (E.On0, E.TF, E.Wk1, E.Tx, E.Sq, E.Wq1, E.On1, E.Sh0, E.Ox0, E.Sh1, E.Sk, E.Wk3, E.Od0, E.Oy0, E.Wk2, E.Oy1, E.On3, E.Pk, E.Wq3, E.Wq2, E.On2, E.Pq, E.Ox1,),
        (E.Sh2, E.K1,),
        (E.Od1,),
        (E.Od3, E.K2, E.Kp,),
        (),
        (E.Oy2, E.Ox2,),
        (E.Od2, E.Sh3,),
        (E.Ox3,),
        (),
    ),
    (1, 1): (
        (E.W0k, E.Ty, E.On0, E.Tp, E.Tx, E.Oy3, E.W0q, E.Od3, E.Sh0,),
        (E.Sk, E.Wk1, E.On1, E.On3, E.TF, E.Wk3, E.Wk2, E.Sq,),
        (E.Sh1, E.Wq1, E.Ox1, E.Pk, E.Wq2,),
        (E.Oy1, E.Ox0, E.On2, E.Ox3, E.K2, E.Wq3, E.Pq, E.Sh2,),
        (E.K1, E.Kp, E.Od1,),
        (),
        (E.Oy0, E.Ox2, E.Sh3, E.Oy2, E.Od0,),
        (),
        (E.Od2,),
        (),
    ),
    (2, 0): (
        (E.Oy3, E.Ty, E.Tp, E.W0k, E.On0, E.W0q, E.Ox3, E.Wk1, E.On3, E.TF, E.Tx, E.Sh0,),
        (E.Sk, E.On1, E.Wk3, E.Wk2, E.Sh1, E.Wq2, E.Wq1, E.Oy0,),
        (E.Oy1, E.On2, E.Ox1, E.Pk, E.Ox0, E.Sq,),
        (E.Sh2, E.Wq3, E.Pq, E.K2, E.Od0,),
        (E.K1, E.Kp, E.Od1, E.Od3, E.Oy2, E.Ox2,),
        (E.Sh3,),
        (),
        (),
        (E.Od2,),
        (),
    ),
    (2, 1): (
        (E.Oy3, E.Ty, E.W0k, E.Tx, E.Tp, E.On0, E.Sh0, E.W0q, E.Sk, E.TF, E.Wk1, E.On1, E.Sh1,),
        (E.Wk2, E.Ox0, E.On3, E.Wk3,),
        (E.Sq, E.Wq1, E.Wq3, E.Pk, E.Wq2, E.Oy1, E.Pq,),
        (E.Ox1, E.Od0, E.On2, E.K1,),
        (E.Sh2, E.Oy0, E.K2, E.Kp, E.Od3,),
        (E.Ox2, E.Od1, E.Od2, E.Ox3, E.Oy2,),
        (),
        (),
        (),
        (E.Sh3,),
    ),
    (3, 0): (
        (E.W0k, E.Tp, E.Wk1, E.On0,),
        (E.Ty, E.Sh0, E.W0q, E.Tx, E.On1, E.TF, E.Sh1, E.On2,),
        (E.Wq1, E.Wk3, E.Sh2, E.Wk2, E.Sq, E.Oy1, E.Oy0, E.Ox0, E.Ox1, E.Wq3, E.On3, E.Sk, E.Sh3, E.Ox2, E.Pk, E.K1,),
        (E.Od0, E.Oy3, E.Wq2, E.Oy2, E.Pq, E.K2, E.Kp,),
        (E.Od2,),
        (E.Od1,),
        (),
        (E.Ox3,),
        (),
        (E.Od3,),
    ),
    (3, 1): (
        (),
        (E.W0k, E.Ty, E.On0, E.Tp, E.Tx, E.W0q, E.Sh0, E.TF, E.On1, E.Wk2, E.Sk, E.On2, E.Sh1, E.Sq, E.Ox0, E.Wk1, E.Sh2, E.Oy2, E.Wk3, E.Pk, E.Ox1, E.Oy0, E.Wq2, E.Od0,),
        (E.Oy1, E.Ox2, E.Wq1, E.Wq3,),
        (E.On3, E.Pq, E.Sh3, E.K1,),
        (E.K2, E.Kp, E.Od1, E.Od2,),
        (E.Oy3, E.Ox3, E.Od3,),
        (),
        (),
        (),
        (),
    ),
}


def fits(mesh, tokens, w_key, w_out):
    seq, head = mesh.shape["seq"], mesh.shape["head"]
    width = tokens[1]
    weights = 2 * width * (w_key[1] // head) * (GROUP + 2)
    outs = 2 * w_out[0] * width
    rows = tokens[0] // seq
    rest = rows * width * (4 + 2 + 4 + 2) + tokens[0] * (w_key[1] // head) * 4
    return (
        head == 4
        and seq == 2 * LINE
        and w_key[1] // head == HD
        and (width // head) % 128 == 0
        and (width // seq) % (16 * PIECES) == 0
        and weights + outs + rest < 44 * 2**20
    )


def sides(z, k, down=True):
    return [z] if k == 0 else [at for at in (z - k, z + k if down else -1) if 0 <= at < LINE]


class Moves:
    def __init__(self, z, kind, e):
        self.z, self.kind, self.e = z, kind, e
        x, y = e.x, e.y
        c = x if kind == 0 else 1 - x
        self.x, self.y, self.c = x, y, c
        self.me, self.head = 2 * z + x, 2 * y + c
        self.partner = (self.me, 2 * y + 1 - c)
        self.xn = (2 * z + 1 - x, self.head)
        self.yn = (self.me, 2 * (1 - y) + c)
        self.hg = 2 * y + x

    def remote(self, src, dst, send, recv, where):
        return pltpu.make_async_remote_copy(
            src_ref=src, dst_ref=dst, send_sem=send, recv_sem=recv,
            device_id=where, device_id_type=MESH,
        )

    def w_ref(self, b, part):
        e = self.e
        rows = pl.ds(pl.multiple_of(b * e.deep, 16), e.deep)
        return e.W.at[rows, pl.ds(part * e.qd, e.qd)]

    def w_copy(self, part, zz, way):
        e = self.e
        b = 2 * zz + self.c
        where = ((self.me + 2, self.head), (self.me - 2, self.head), self.partner)[way]
        ref = self.w_ref(b, part)
        return self.remote(ref, ref, e.w_send, e.w_recv.at[part, LINE if way == 2 else zz], where)

    def w_onward(self, part, zz):
        return [
            self.w_copy(part, zz, way)
            for way, told in (
                (0, zz <= self.z < LINE - 1), (1, zz >= self.z > 0), (2, True),
            )
            if told
        ]

    def w_swap(self, part):
        e = self.e
        return self.remote(
            e.SW.at[:, pl.ds(part * e.qd, e.qd)], self.w_ref(self.me, part),
            e.w_send, e.w_recv.at[part, self.z], (2 * self.z + self.c, self.hg),
        )

    def w_take(self, part, zz):
        self.remote_take(self.w_ref(2 * zz + self.c, part), self.e.w_recv.at[part, zz])

    def w_beside(self, part):
        self.remote_take(self.units(LINE), self.e.w_recv.at[part, LINE])

    def units(self, n):
        return self.e.WO.at[pl.ds(0, n * self.e.deep)]

    def remote_take(self, ref, recv):
        self.remote(ref, ref, self.e.w_send, recv, self.partner).wait_recv()

    def remote_left(self, ref, send):
        self.remote(ref, ref, send, self.e.w_recv.at[0, 0], self.partner).wait_send()

    def k_copy(self, zz, way):
        e = self.e
        b = 2 * zz + self.c
        where = ((self.me + 2, self.head), self.partner)[way]
        return self.remote(e.KV.at[b], e.KV.at[b], e.k_send, e.k_recv.at[LINE if way else zz], where)

    def k_onward(self, zz):
        up = zz <= self.z < LINE - 1 and self.z - zz < REACH
        return ([self.k_copy(zz, 0)] if up else []) + [self.k_copy(zz, 1)]

    def k_take(self, zz):
        self.remote_take(self.e.KV.at[2 * zz + self.c], self.e.k_recv.at[zz])

    def k_beside(self):
        n = self.z + 1 - max(self.z - REACH, 0)
        self.remote_take(self.e.KV.at[pl.ds(0, n)], self.e.k_recv.at[LINE])

    def t_copy(self, way):
        e = self.e
        where = (
            self.partner,
            (2 * self.z + 1 - self.x, 2 * self.y + self.x),
            (self.me, 2 * (1 - self.y) + self.x),
        )[way]
        return self.remote(e.TOK, e.X.at[0, self.head], e.t_send, e.t_recv.at[self.head], where)

    def t_take(self, h):
        self.remote_take(self.e.X.at[0, h], self.e.t_recv.at[h])

    def t_relay(self):
        e = self.e
        h, where = ((2 * (1 - self.y) + self.x, self.xn), (2 * self.y + self.x, self.yn))[self.kind]
        return h, self.remote(e.X.at[0, h], e.X.at[0, h], e.t_send, e.t_recv.at[h], where)

    def r_copy(self, h):
        e = self.e
        return self.remote(e.X.at[0, h], e.X.at[1, h], e.r_send, e.r_recv, self.partner)

    def o_copy(self, way, zz, fx, fy, i):
        e = self.e
        b = 2 * zz + (1 - self.x if fx else self.x)
        h = 2 * (1 - self.y) + self.c if fy else self.head
        if way == "c":
            send, recv, where = e.oc_send, e.o_side.at[zz], self.partner
        else:
            fx, fy, where = {
                "up": (fx, fy, (self.me + 2, self.head)),
                "down": (fx, fy, (self.me - 2, self.head)),
                "x": (1, fy, self.xn),
                "y": (fx, 1, self.yn),
            }[way]
            send, recv = e.o_send, e.o_recv.at[2 * fx + fy, zz, i]
        ref = self.o_ref(b, h, i)
        return self.remote(ref, ref, send, recv, where)

    def o_ref(self, b, h, i):
        e = self.e
        piece = e.deep // PIECES
        at = (h * 2 * LINE + b) * e.deep + i * piece
        return e.WO.at[pl.ds(pl.multiple_of(at, 16), piece)]

    def o_onward(self, zz, i):
        return [
            self.o_copy(way, zz, 0, 0, i)
            for way, told in (("up", zz <= self.z < LINE - 1), ("down", zz >= self.z > 0))
            if told
        ]

    def o_share(self, zz, i):
        return [self.o_copy(way, zz, 0, 0, i) for way in ("x", "y", "c")]

    def o_from_x(self, zz, i):
        turn = [self.o_copy("y", zz, 1, 0, i)] if zz not in OVER_X else []
        return turn + [self.o_copy("c", zz, 1, 0, i)]

    def o_from_y(self, zz, i):
        turn = [self.o_copy("x", zz, 0, 1, i)] if zz in OVER_X else []
        return turn + [self.o_copy("c", zz, 0, 1, i)]

    def o_take(self, zz, fx, fy, i):
        self.remote_take(self.o_ref(0, 0, i), self.e.o_recv.at[2 * fx + fy, zz, i])

    def o_beside(self, zz):
        self.remote_take(self.units(4), self.e.o_side.at[zz])

    def a_copy(self, way):
        e = self.e
        where = (
            self.partner, self.yn, self.xn, (2 * self.z + 1 - self.x, 2 * (1 - self.y) + self.c),
        )[way]
        return self.remote(e.AO, e.ATT.at[self.hg], e.a_send, e.a_recv.at[0 if way == 0 else self.hg], where)

    def a_ways(self):
        return (1, 0) if self.kind == 0 else (2, 3)

    def a_pass(self, h):
        e = self.e
        return self.remote(e.ATT.at[h], e.ATT.at[h], e.a_send, e.a_recv.at[0], self.partner)

    def a_far(self):
        x, y = self.x, self.y
        return (2 * (1 - y) + x, 2 * y + 1 - x, 2 * (1 - y) + 1 - x)

    def do(self, event):
        z, kind, e = self.z, self.kind, self.e
        event = event.name
        name, k = event[:-1], event[-1]
        begin = lambda copies: [copy.start() for copy in copies]
        if name == "W0":
            part = "qk".index(k)
            for move in e.w_loads[kind][part]:
                move.wait()
            begin(self.w_onward(part, z) if kind == 0 else [self.w_swap(part)])
        elif name == "S":
            if kind == 1:
                part = "qk".index(k)
                self.w_take(part, z)
                begin(self.w_onward(part, z))
        elif name in ("Wq", "Wk"):
            part = "qk".index(name[1])
            for zz in sides(z, int(k)):
                self.w_take(part, zz)
                begin(self.w_onward(part, zz))
        elif name == "P":
            self.w_beside("qk".index(k))
        elif event in ("Tp", "Tx", "Ty"):
            if (z, kind) not in e.loaded:
                e.loaded.add((z, kind))
                e.l_tok.wait()
            if event != "Tp" or kind == 1:
                self.t_copy("pxy".index(event[1])).start()
        elif event == "TF":
            h, relay = self.t_relay()
            self.t_take(h)
            relay.start()
        elif name == "On":
            for zz in sides(z, int(k)):
                for i in range(PIECES):
                    if zz != z:
                        self.o_take(zz, 0, 0, i)
                    elif i == 0:
                        e.l_out.wait()
                    begin(self.o_onward(zz, i))
        elif name == "Sh":
            for zz in sides(z, int(k)):
                for i in range(PIECES):
                    begin(self.o_share(zz, i))
        elif name in ("Ox", "Oy", "Od"):
            fx, fy = {"x": (1, 0), "y": (0, 1), "d": (1, 1)}[name[1]]
            for zz in sides(z, int(k)):
                for i in range(PIECES):
                    self.o_take(zz, fx, fy, i)
                    if fx and fy:
                        self.o_copy("c", zz, 1, 1, i).start()
                    else:
                        begin(self.o_from_x(zz, i) if fx else self.o_from_y(zz, i))
        elif event == "Kp":
            self.k_beside()
        elif name == "K":
            for zz in sides(z, int(k), False):
                self.k_take(zz)
                begin(self.k_onward(zz))
        else:
            raise ValueError(event)

    def tokens(self):
        e = self.e
        x, y = self.x, self.y
        if self.kind == 0:
            e.l_own.wait()
            self.t_take(2 * y + 1 - x)
            self.t_take(2 * (1 - y) + 1 - x)
            for h in range(4):
                self.r_copy(h).start()
        else:
            self.t_take(2 * y + 1 - x)
            self.t_take(2 * (1 - y))
            self.t_take(2 * (1 - y) + 1)

    def attended(self):
        for way in self.a_ways():
            self.a_copy(way).start()

    def gathered(self):
        e = self.e
        if self.kind == 0:
            for h in self.a_far():
                self.remote_take(e.ATT.at[h], e.a_recv.at[h])
                self.a_pass(h).start()
        else:
            self.remote_take(e.ATT, e.a_recv.at[0])
            self.remote_take(e.X.at[1], e.r_recv)

    def emitted(self, k):
        for zz in sides(self.z, k):
            self.o_beside(zz)

    def drain(self):
        z, kind, e = self.z, self.kind, self.e
        weights = sum(len(self.w_onward(part, zz)) for part in range(2) for zz in range(LINE))
        self.remote_left(self.units(weights + 2 * kind), e.w_send)
        outs = sum(
            len(self.o_onward(zz, 0)) + 2 + len(self.o_from_x(zz, 0)) + len(self.o_from_y(zz, 0)) - 2
            for zz in range(LINE)
        )
        self.remote_left(self.units(outs), e.o_send)
        self.remote_left(self.units(4 * LINE), e.oc_send)
        keys = sum(len(self.k_onward(zz)) for zz in range(max(z - REACH, 0), z + 1))
        self.remote_left(e.KV.at[pl.ds(0, keys)], e.k_send)
        self.remote_left(e.X.at[0, pl.ds(0, 3 + kind)], e.t_send)
        self.remote_left(e.KV.at[pl.ds(0, 2 if kind else 5)], e.a_send)
        if kind == 0:
            self.remote_left(e.X.at[0], e.r_send)


class Names:
    pass


def kernel(
    seq, heads, rows, width, most,
    tok, seg_row, wq, wk, wv, wo_in, pre_in, post_in, freq_in,
    out,
    TOK, X, XN, SW, W, WO, SEG, KV, AO, ATT, PR, RQ, NUM, DEN, pre1, post1, pre, post, freq,
    loc, t_recv, t_send, r_recv, r_send, s_recv, s_send, w_recv, w_send,
    o_recv, o_side, o_send, oc_send, k_recv, k_send, a_recv, a_send,
):
    me, head = lax.axis_index("seq"), lax.axis_index("head")
    z, x = me // 2, lax.rem(me, 2)
    y, c = head // 2, lax.rem(head, 2)
    deep = width // seq
    cut = width // heads
    qd, kd = wq.shape[1], wk.shape[1]
    same = c == x
    other = c != x
    rb = 2 * z + c
    hg = 2 * y + x

    e = Names()
    e.x, e.y, e.deep, e.qd = x, y, deep, qd
    e.loaded = set()
    e.TOK, e.X, e.SW, e.W, e.WO, e.KV, e.AO, e.ATT = TOK, X, SW, W, WO, KV, AO, ATT
    e.t_recv, e.t_send, e.r_recv, e.r_send = t_recv, t_send, r_recv, r_send
    e.w_recv, e.w_send, e.o_recv, e.o_side = w_recv, w_send, o_recv, o_side
    e.o_send, e.oc_send = o_send, oc_send
    e.k_recv, e.k_send, e.a_recv, e.a_send = k_recv, k_send, a_recv, a_send

    def load_weights(block):
        return (
            [pltpu.make_async_copy(wq, block.at[:, pl.ds(0, qd)], loc.at[4])],
            [
                pltpu.make_async_copy(wk, block.at[:, pl.ds(qd, kd)], loc.at[5]),
                pltpu.make_async_copy(wv, block.at[:, pl.ds(qd + kd, kd)], loc.at[6]),
            ],
        )

    mine = pl.ds(pl.multiple_of(me * deep, 16), deep)
    e.w_loads = (load_weights(W.at[mine]), load_weights(SW))
    e.l_tok = pltpu.make_async_copy(tok, TOK, loc.at[0])
    e.l_own = pltpu.make_async_copy(tok, X.at[0, head], loc.at[1])
    l_seg = pltpu.make_async_copy(seg_row, SEG.at[me], loc.at[2])
    place = pl.ds(pl.multiple_of((head * seq + me) * deep, 16), deep)
    e.l_out = pltpu.make_async_copy(wo_in, WO.at[place], loc.at[3])
    small = [
        pltpu.make_async_copy(pre_in, pre1, loc.at[7]),
        pltpu.make_async_copy(post_in, post1, loc.at[8]),
        pltpu.make_async_copy(freq_in, freq, loc.at[9]),
    ]

    for kind, told in enumerate((same, other)):
        @pl.when(told)
        def _():
            for part in (1, 0):
                for move in e.w_loads[kind][part]:
                    move.start()

    l_seg.start()
    e.l_tok.start()
    e.l_out.start()

    @pl.when(same)
    def _():
        e.l_own.start()

    for move in small:
        move.start()

    barrier = pltpu.get_barrier_semaphore()

    def greet(where):
        pl.semaphore_signal(barrier, inc=1, device_id=where, device_id_type=MESH)

    for dx in range(2):
        for dy in range(2):
            for dc in range(2):
                if dy + dc > 0:
                    gx = lax.rem(x + dx, 2)
                    greet((2 * z + gx, 2 * lax.rem(y + dy, 2) + lax.rem(c + dc, 2)))
    for d in range(1, seq):
        greet((lax.rem(me + d, seq), head))
    pl.semaphore_wait(barrier, 6 + seq - 1)

    l_seg.wait()

    def s_copy(d):
        return pltpu.make_async_remote_copy(
            src_ref=SEG.at[me], dst_ref=SEG.at[me], send_sem=s_send, recv_sem=s_recv,
            device_id=(lax.rem(me + d, seq), head), device_id_type=MESH,
        )

    def s_all():
        ref = SEG.at[pl.ds(0, seq - 1)]
        return pltpu.make_async_remote_copy(
            src_ref=ref, dst_ref=ref, send_sem=s_send, recv_sem=s_recv,
            device_id=(lax.rem(me + 1, seq), head), device_id_type=MESH,
        )

    for d in range(1, seq):
        s_copy(d).start()

    def everyone(act):
        for place in range(LINE):
            for kind, told in enumerate((same, other)):
                @pl.when((z == place) & told)
                def _():
                    act(Moves(place, kind, e))

    def events(phase):
        def act(moves):
            for event in PLAN[moves.z, moves.kind][phase]:
                moves.do(event)

        everyone(act)

    events(0)
    s_all().wait_recv()
    for move in small:
        move.wait()
    for h in range(heads):
        at = slice(h * cut, (h + 1) * cut)
        pre[0:1, at] = pre1[at][None, :]
        post[0:1, at] = post1[at][None, :]
    own = jnp.broadcast_to(SEG[rb].astype(F32), (HD, rows))
    col = jnp.transpose(own)[:, 0:1]
    start = jnp.zeros((rows, 1), F32)
    for j in range(seq):
        start += jnp.sum((SEG[j].astype(F32) < col).astype(F32), axis=1, keepdims=True)
    index = (rb * rows + lax.broadcasted_iota(jnp.int32, (rows, 1), 0)).astype(F32)
    angle = (index - start) * freq[...]
    cosine = jnp.cos(angle)
    sine = jnp.sin(angle)
    lane = lax.broadcasted_iota(jnp.int32, (rows, HD), 1)
    sine = jnp.where(lane < HD // 2, -sine, sine)

    events(1)
    everyone(lambda moves: moves.tokens())
    half = rows // 2

    def norm_rows(r, _):
        at = pl.ds(pl.multiple_of(r * half, half), half)
        total = jnp.zeros((half, 1), F32)
        for h in range(heads):
            wide = X[0, h, at, :].astype(F32)
            total += jnp.sum(wide * wide, axis=1, keepdims=True)
        scale = lax.rsqrt(total / width + EPS)
        for h in range(heads):
            gain = pre[0:1, h * cut : (h + 1) * cut]
            XN[h, at, :] = (X[0, h, at, :].astype(F32) * scale * gain).astype(BF16)
        return 0

    lax.fori_loop(0, 2, norm_rows, 0)

    def project(part):
        cols = slice(part * qd, (part + 1) * qd)
        total = jnp.zeros((rows, qd), F32)
        for h in range(heads):
            some = slice(h * cut, (h + 1) * cut)
            total += jnp.dot(XN[h], W[some, cols], preferred_element_type=F32)
        return total

    def turn(values):
        return values * cosine + pltpu.roll(values, HD // 2, 1) * sine

    events(2)
    keyed = project(1)
    KV[rb, :, 0:HD] = turn(keyed[:, 0:HD]).astype(BF16)
    KV[rb, :, HD : 2 * HD] = keyed[:, kd : kd + HD].astype(BF16)
    everyone(lambda moves: [copy.start() for copy in moves.k_onward(moves.z)])
    events(3)
    asked = project(0)
    for g in range(GROUP):
        RQ[g * rows : (g + 1) * rows, :] = (
            turn(asked[:, g * HD : (g + 1) * HD]) * SCALAR ** (-0.5)
        ).astype(BF16)

    events(4)
    start2 = jnp.concatenate([start] * GROUP, axis=0)
    index2 = jnp.concatenate([index] * GROUP, axis=0)
    NUM[...] = jnp.zeros_like(NUM)
    DEN[...] = jnp.zeros_like(DEN)

    def attend(j, _):
        s = lax.dot_general(
            RQ[...], KV[j, :, 0:HD], (((1,), (1,)), ((), ())), preferred_element_type=F32
        )
        at = (j * rows + lax.broadcasted_iota(jnp.int32, (1, rows), 1)).astype(F32)
        p = jnp.where(
            (at >= start2) & (at <= index2), jnp.exp(CAP * jnp.tanh(s * (1.0 / CAP))), 0.0
        )
        DEN[...] += jnp.sum(p, axis=1, keepdims=True)
        NUM[...] += jnp.dot(p.astype(BF16), KV[j, :, HD : 2 * HD], preferred_element_type=F32)
        return 0

    lax.fori_loop(jnp.maximum(rb - most // rows, 0), rb + 1, attend, 0)
    ratio = (NUM[...] / DEN[:, 0:1]).astype(BF16)
    for g in range(GROUP):
        AO[:, g * HD : (g + 1) * HD] = ratio[g * rows : (g + 1) * rows, :]
    everyone(lambda moves: moves.attended())

    @pl.when(same)
    def _():
        for g in range(GROUP):
            ATT[hg, :, g * HD : (g + 1) * HD] = ratio[g * rows : (g + 1) * rows, :]

    events(5)
    everyone(lambda moves: moves.gathered())

    def emit(n):
        acc = jnp.zeros((rows, cut), F32)
        for h in range(heads):
            acc += lax.dot_general(
                ATT[h], WO[pl.ds(pl.multiple_of(h * width + n * cut, 128), cut), :],
                (((1,), (1,)), ((), ())), preferred_element_type=F32,
            )
        PR[n] = acc
        DEN[0:rows, 0:1] += jnp.sum(acc * acc, axis=1, keepdims=True)

    DEN[...] = jnp.zeros_like(DEN)
    for k in range(LINE):
        events(6 + k)
        everyone(lambda moves: moves.emitted(k))
        if k == 0:
            emit(z)
        else:

            @pl.when(z >= k)
            def _():
                emit(z - k)

            @pl.when(z + k < LINE)
            def _():
                emit(z + k)
    scale = lax.rsqrt(DEN[0:rows, 0:1] / width + EPS)
    kept = other.astype(jnp.int32)

    def finish(h, _):
        at = pl.ds(pl.multiple_of(h * cut, 128), cut)
        out[:, at] = (X[kept, h].astype(F32) + PR[h] * scale * post[0:1, at]).astype(BF16)
        return 0

    lax.fori_loop(0, heads, finish, 0)
    everyone(lambda moves: moves.drain())
    s_all().wait_send()


def fused(tokens, segments, pre_gain, post_gain, w_query, w_key, w_value, w_out):
    seq, heads = lax.axis_size("seq"), lax.axis_size("head")
    rows, cut = tokens.shape
    width = cut * heads
    deep = width // seq
    qd, kd = w_query.shape[1], w_key.shape[1]
    most = rows * seq // 2
    half = HD // 2
    freq = np.float32(10000.0) ** (-(np.arange(half, dtype=np.float32) / np.float32(half)))
    freq = np.concatenate([freq, freq])[None, :].astype(np.float32)
    hbm = pl.BlockSpec(memory_space=pl.ANY)
    vmem = pl.BlockSpec(memory_space=pltpu.VMEM)
    dma = pltpu.SemaphoreType.DMA
    return pl.pallas_call(
        functools.partial(kernel, seq, heads, rows, width, most),
        out_shape=pltpu.VMEM((rows, width), BF16),
        in_specs=[hbm] * 9,
        out_specs=vmem,
        scratch_shapes=[
            pltpu.VMEM((rows, cut), BF16),
            pltpu.VMEM((2, heads, rows, cut), BF16),
            pltpu.VMEM((heads, rows, cut), BF16),
            pltpu.VMEM((deep, qd + 2 * kd), BF16),
            pltpu.VMEM((width, qd + 2 * kd), BF16),
            pltpu.VMEM((heads * width, w_out.shape[0]), BF16),
            pltpu.VMEM((seq, 1, rows), jnp.int32),
            pltpu.VMEM((seq, rows, 2 * HD), BF16),
            pltpu.VMEM((rows, GROUP * HD), BF16),
            pltpu.VMEM((heads, rows, GROUP * HD), BF16),
            pltpu.VMEM((heads, rows, cut), F32),
            pltpu.VMEM((GROUP * rows, HD), BF16),
            pltpu.VMEM((GROUP * rows, HD), F32),
            pltpu.VMEM((GROUP * rows, HD), F32),
            pltpu.VMEM((width,), F32),
            pltpu.VMEM((width,), F32),
            pltpu.VMEM((1, width), F32),
            pltpu.VMEM((1, width), F32),
            pltpu.VMEM((1, HD), F32),
            dma((10,)),
            dma((heads,)), dma, dma, dma, dma, dma,
            dma((2, LINE + 1)), dma,
            dma((4, LINE, PIECES)), dma((LINE,)), dma, dma,
            dma((LINE + 1,)), dma, dma((heads,)), dma,
        ],
        compiler_params=pltpu.CompilerParams(
            collective_id=0, has_side_effects=True, vmem_limit_bytes=52 * 2**20
        ),
    )(
        tokens, segments[None, :], w_query, w_key, w_value, w_out.T,
        pre_gain, post_gain, freq,
    )


def solution(mesh):
    specs = (
        P("seq", "head"),
        P("seq"),
        P(),
        P(),
        P("seq", "head"),
        P("seq", "head"),
        P("seq", "head"),
        P("head", "seq"),
    )

    def run(*args):
        small = fits(mesh, args[0].shape, args[5].shape, args[7].shape)
        return jax.shard_map(
            fused if small else local,
            mesh=mesh,
            in_specs=specs,
            out_specs=P("seq", None),
            check_vma=False,
        )(*args)

    return run
```

```python
import enum
import functools

import jax
import jax.numpy as jnp
import numpy as np
from jax import lax
from jax.experimental import pallas as pl
from jax.experimental.pallas import tpu as pltpu
from jax.sharding import PartitionSpec as P

HD = 128
GROUP = 2
SCALAR = 144
DOCS = 8


EPS = 1e-06
CAP = 50.0


def carried_in(value, axis, join, neutral):
    count, mine = (lax.axis_size(axis), lax.axis_index(axis))
    pieces = lax.all_gather(value, axis)
    subtotal = jnp.full_like(value, 0) + jnp.asarray(neutral, value.dtype)

    def step(position, subtotal):
        longer = join(subtotal, pieces[position])
        return jnp.where(position < mine, longer, subtotal)

    return lax.fori_loop(0, count - 1, step, subtotal)


def rotate(values, position, width):
    count = values.shape[1] // width
    half = width // 2
    shaped = values.reshape(values.shape[0], count, width)
    freq = 10000.0 ** (-(jnp.arange(half, dtype=jnp.float32) / half))
    angle = position[:, None] * freq[None, :]
    cosine = jnp.cos(angle)[:, None, :]
    sine = jnp.sin(angle)[:, None, :]
    first = shaped[:, :, :half]
    second = shaped[:, :, half:]
    turned = jnp.concatenate(
        [first * cosine - second * sine, second * cosine + first * sine], axis=2
    )
    return turned.reshape(values.shape[0], count * width)


def add_counts(earlier, later):
    return earlier + later


def local(tokens, segments, pre_gain, post_gain, w_query, w_key, w_value, w_out):
    rows = tokens.shape[0]
    whole = lax.all_gather(tokens, "head", axis=1, tiled=True)
    wide = whole.astype(jnp.float32)
    normed = (
        wide * lax.rsqrt(jnp.mean(wide * wide, axis=1, keepdims=True) + EPS) * pre_gain
    ).astype(jnp.bfloat16)
    pieces = (
        lax.all_gather(w_query, "seq", axis=0, tiled=True),
        lax.all_gather(w_key, "seq", axis=0, tiled=True),
        lax.all_gather(w_value, "seq", axis=0, tiled=True),
    )
    query, key_proj, value_proj = tuple(
        (jnp.dot(normed, piece, preferred_element_type=jnp.float32) for piece in pieces)
    )
    levels = jnp.arange(DOCS, dtype=jnp.int32)
    below = jnp.sum((levels[None, :] > segments[:, None]).astype(jnp.float32), axis=0)
    earlier = carried_in(below, "seq", add_counts, jnp.zeros((DOCS,), jnp.float32))
    starts = earlier + below
    onehot = (segments[:, None] == levels[None, :]).astype(jnp.float32)
    tok_start = jnp.sum(onehot * starts[None, :], axis=1)
    offset = lax.axis_index("seq") * rows
    index_f = (offset + jnp.arange(rows, dtype=jnp.int32)).astype(jnp.float32)
    position = index_f - tok_start
    kv_count = w_key.shape[1] // HD
    rq = (rotate(query, position, HD) * SCALAR ** (-0.5)).astype(jnp.bfloat16)
    rk = rotate(key_proj, position, HD).astype(jnp.bfloat16)
    vb = value_proj.astype(jnp.bfloat16)
    stacked = (
        rq.reshape(rows, kv_count, GROUP, HD)
        .transpose(1, 2, 0, 3)
        .reshape(kv_count, GROUP * rows, HD)
    )
    query_start = jnp.tile(tok_start, GROUP)
    query_index = jnp.tile(index_f, GROUP)
    empty = (
        jnp.zeros((kv_count, GROUP * rows, HD), jnp.float32),
        jnp.zeros((kv_count, GROUP * rows), jnp.float32),
    )
    keys_all = lax.all_gather(rk, "seq", axis=0, tiled=True)
    values_all = lax.all_gather(vb, "seq", axis=0, tiled=True)
    count = keys_all.shape[0]
    block = 1024
    steps_total = count // block

    def compute(offset_blk, state):
        numer, denom = state
        keys_blk = lax.dynamic_slice_in_dim(keys_all, offset_blk, block, 0).reshape(
            block, kv_count, HD
        )
        values_blk = lax.dynamic_slice_in_dim(values_all, offset_blk, block, 0).reshape(
            block, kv_count, HD
        )
        key_index = (offset_blk + jnp.arange(block, dtype=jnp.int32)).astype(jnp.float32)
        scores = jnp.einsum("cqd,kcd->cqk", stacked, keys_blk, preferred_element_type=jnp.float32)
        capped = CAP * jnp.tanh(scores / CAP)
        allowed = (key_index[None, None, :] >= query_start[None, :, None]) & (
            key_index[None, None, :] <= query_index[None, :, None]
        )
        weights = jnp.where(allowed, jnp.exp(capped), 0.0)
        numer = numer + jnp.einsum(
            "cqk,kcd->cqd",
            weights.astype(jnp.bfloat16),
            values_blk,
            preferred_element_type=jnp.float32,
        )
        denom = denom + jnp.sum(weights, axis=2)
        return (numer, denom)

    def one_block(step, state):
        offset_blk = step * block
        return compute(offset_blk, state)

    numer, denom = lax.fori_loop(0, steps_total, one_block, empty)
    attn = (numer / denom[:, :, None]).reshape(kv_count, GROUP, rows, HD).transpose(2, 0, 1, 3)
    attn = attn.reshape(rows, kv_count * GROUP * HD).astype(jnp.bfloat16)
    partial_proj = jnp.dot(
        attn, lax.all_gather(w_out, "seq", axis=1, tiled=True), preferred_element_type=jnp.float32
    )
    partial_proj = lax.optimization_barrier(partial_proj.astype(jnp.bfloat16)).astype(jnp.float32)
    summed = lax.psum(partial_proj.astype(jnp.bfloat16), "head").astype(jnp.float32)
    scale = lax.rsqrt(jnp.mean(summed * summed, axis=1, keepdims=True) + EPS)
    return (wide + summed * scale * post_gain).astype(jnp.bfloat16)


MESH = pl.DeviceIdType.MESH
BF16 = jnp.bfloat16
F32 = jnp.float32
LINE = 4
REACH = LINE // 2
PIECES = 1
OVER_X = (0,)

class E(enum.Enum):
    K1 = enum.auto()
    K2 = enum.auto()
    Kp = enum.auto()
    Od0 = enum.auto()
    Od1 = enum.auto()
    Od2 = enum.auto()
    Od3 = enum.auto()
    On0 = enum.auto()
    On1 = enum.auto()
    On2 = enum.auto()
    On3 = enum.auto()
    Ox0 = enum.auto()
    Ox1 = enum.auto()
    Ox2 = enum.auto()
    Ox3 = enum.auto()
    Oy0 = enum.auto()
    Oy1 = enum.auto()
    Oy2 = enum.auto()
    Oy3 = enum.auto()
    Sh0 = enum.auto()
    Sh1 = enum.auto()
    Sh2 = enum.auto()
    Sh3 = enum.auto()
    Sk = enum.auto()
    Sq = enum.auto()
    TF = enum.auto()
    Tp = enum.auto()
    Tx = enum.auto()
    Ty = enum.auto()
    W0k = enum.auto()
    W0q = enum.auto()
    Wk1 = enum.auto()
    Wk2 = enum.auto()
    Wk3 = enum.auto()
    Wq1 = enum.auto()
    Wq2 = enum.auto()
    Wq3 = enum.auto()


PLAN = {
    (0, 0): (
        (E.On0, E.Tp, E.Ty, E.Tx, E.W0q, E.W0k, E.On1, E.Sh1, E.On2, E.TF, E.Sh0, E.Ox1, E.Wk1,),
        (E.Sk, E.Wq1, E.On3, E.Sh2,),
        (E.Wk2, E.Sh3, E.Sq, E.Wk3,),
        (),
        (),
        (),
        (E.Oy0, E.Ox2, E.Wq2, E.Wq3,),
        (E.K1, E.Od1, E.K2, E.Ox0, E.Od0,),
        (),
        (),
        (E.Oy1, E.Od2, E.Kp,),
        (E.Oy2, E.Oy3,),
        (E.Ox3,),
        (),
        (E.Od3,),
        (),
    ),
    (0, 1): (
        (E.On0, E.Tp, E.W0k, E.Ty, E.W0q, E.Sq, E.Sh0, E.On2, E.Sk, E.Wq1, E.Tx, E.On1, E.Ox1, E.Sh1, E.Oy1, E.TF, E.Sh2, E.Wk1, E.Wk3, E.Ox2, E.Oy0,),
        (E.Wk2, E.Oy2,),
        (E.Wq2,),
        (),
        (E.On3, E.Od1,),
        (E.Od2, E.Ox0, E.K2, E.K1, E.Wq3,),
        (),
        (E.Ox3,),
        (E.Od0, E.Sh3,),
        (E.Kp,),
        (),
        (),
        (),
        (E.Oy3, E.Od3,),
        (),
        (),
    ),
    (1, 0): (
        (E.Wq3, E.Tp, E.On0, E.Ty, E.Wk3, E.Wk1, E.Ox0, E.W0k, E.Ox3, E.Sh0, E.On1, E.Oy3, E.TF, E.Tx, E.Od0, E.Sh1, E.On2, E.Sh2, E.Wq1, E.W0q, E.Wk2, E.Oy1,),
        (),
        (E.Sk, E.Sq, E.Ox2,),
        (E.Wq2, E.On3, E.Oy0, E.K1, E.Sh3, E.Od3,),
        (),
        (E.K2,),
        (E.Oy2, E.Od2,),
        (E.Kp, E.Ox1,),
        (),
        (),
        (),
        (E.Od1,),
        (),
        (),
        (),
        (),
    ),
    (1, 1): (
        (E.On0, E.Wk3, E.W0k, E.Tp, E.Ty, E.W0q, E.Tx, E.Sk, E.Wq3, E.Sq, E.Sh0, E.On1, E.TF, E.Sh1, E.Wk1, E.Wq1,),
        (E.K2, E.Wk2,),
        (),
        (E.Ox3, E.On2, E.Od3, E.Oy3, E.Ox0, E.Sh2,),
        (E.Oy0,),
        (E.Ox1, E.Oy1, E.Wq2,),
        (),
        (E.Ox2,),
        (),
        (E.On3, E.K1, E.Kp, E.Oy2, E.Od1, E.Od0,),
        (E.Od2,),
        (),
        (),
        (E.Sh3,),
        (),
        (),
    ),
    (2, 0): (
        (E.Tp, E.W0k, E.On0, E.Wk3, E.Wq3, E.Ty, E.Sk, E.Oy3, E.TF, E.W0q, E.Tx, E.On1, E.Wk1, E.Sh0, E.Sq, E.On2, E.Sh2, E.Ox0,),
        (E.Ox1, E.Wk2, E.Sh1, E.Wq2, E.Ox3,),
        (E.On3,),
        (),
        (E.Ox2,),
        (),
        (E.Wq1,),
        (E.K2,),
        (E.Oy2,),
        (E.Oy1, E.Oy0, E.Od1, E.Od0,),
        (E.K1, E.Kp,),
        (E.Od2,),
        (),
        (),
        (),
        (E.Od3, E.Sh3,),
    ),
    (2, 1): (
        (E.Oy3, E.Tp, E.On0, E.W0k, E.Ty, E.Wk3, E.Tx, E.W0q, E.On1, E.Sh0, E.TF, E.Sk, E.Sq, E.Sh1, E.Wk2, E.Wk1,),
        (),
        (E.Wq2, E.On2,),
        (E.Wq1, E.Sh2,),
        (E.Ox2,),
        (),
        (E.Ox3, E.Ox1, E.K1, E.On3, E.Ox0, E.Od3,),
        (),
        (E.Oy1, E.Od1, E.Wq3,),
        (E.K2, E.Oy0, E.Oy2, E.Od2, E.Kp, E.Sh3, E.Od0,),
        (),
        (),
        (),
        (),
        (),
        (),
    ),
    (3, 0): (
        (E.Ty, E.Tp, E.On0, E.W0k, E.On1, E.On2, E.W0q, E.Sh0, E.TF, E.Ox0, E.Ox2, E.Wk2, E.Oy0, E.Tx, E.Sh2, E.Sh1, E.On3, E.Wk1, E.Wk3, E.Ox1, E.Wq3, E.Wq1, E.Sh3,),
        (),
        (E.Oy2, E.Od1, E.K1, E.Sk,),
        (),
        (E.Oy3, E.Sq,),
        (E.Wq2, E.Od2, E.Od0, E.Ox3,),
        (),
        (),
        (E.K2,),
        (E.Kp,),
        (E.Oy1,),
        (),
        (),
        (),
        (E.Od3,),
        (),
    ),
    (3, 1): (
        (E.Ty, E.On0, E.Tp, E.W0q, E.Sh0, E.Sq, E.W0k, E.Tx, E.On1, E.On2, E.Sh2, E.Sk, E.Oy0, E.Sh1, E.TF, E.Ox0, E.Wk3, E.Wk1, E.Ox2,),
        (),
        (),
        (E.Oy1, E.Ox3,),
        (E.On3, E.Od0, E.Wq3, E.Sh3, E.Wk2, E.Wq2,),
        (E.Wq1,),
        (E.Oy3, E.Oy2, E.K2,),
        (E.K1,),
        (E.Od2, E.Ox1,),
        (),
        (E.Kp,),
        (E.Od1, E.Od3,),
        (),
        (),
        (),
        (),
    ),
}


def fits(mesh, tokens, w_key, w_out):
    seq, head = mesh.shape["seq"], mesh.shape["head"]
    width = tokens[1]
    weights = 2 * width * (w_key[1] // head) * (GROUP + 2)
    outs = 2 * w_out[0] * width
    rows = tokens[0] // seq
    rest = rows * width * (4 + 2 + 4 + 2) + tokens[0] * (w_key[1] // head) * 4
    return (
        head == 4
        and seq == 2 * LINE
        and w_key[1] // head == HD
        and (width // head) % 128 == 0
        and (width // seq) % (16 * PIECES) == 0
        and weights + outs + rest < 44 * 2**20
    )


def sides(z, k, down=True):
    return [z] if k == 0 else [at for at in (z - k, z + k if down else -1) if 0 <= at < LINE]


class Moves:
    def __init__(self, z, kind, e):
        self.z, self.kind, self.e = z, kind, e
        x, y = e.x, e.y
        c = x if kind == 0 else 1 - x
        self.x, self.y, self.c = x, y, c
        self.me, self.head = 2 * z + x, 2 * y + c
        self.partner = (self.me, 2 * y + 1 - c)
        self.xn = (2 * z + 1 - x, self.head)
        self.yn = (self.me, 2 * (1 - y) + c)
        self.hg = 2 * y + x

    def remote(self, src, dst, send, recv, where):
        return pltpu.make_async_remote_copy(
            src_ref=src, dst_ref=dst, send_sem=send, recv_sem=recv,
            device_id=where, device_id_type=MESH,
        )

    def w_ref(self, b, part):
        e = self.e
        rows = pl.ds(pl.multiple_of(b * e.deep, 16), e.deep)
        return e.W.at[rows, pl.ds(part * e.qd, e.qd)]

    def w_copy(self, part, zz, way):
        e = self.e
        b = 2 * zz + self.c
        where = ((self.me + 2, self.head), (self.me - 2, self.head), self.partner)[way]
        ref = self.w_ref(b, part)
        return self.remote(ref, ref, e.w_send, e.w_recv.at[part, LINE + zz if way == 2 else zz], where)

    def w_onward(self, part, zz):
        return [
            self.w_copy(part, zz, way)
            for way, told in (
                (0, zz <= self.z < LINE - 1), (1, zz >= self.z > 0), (2, True),
            )
            if told
        ]

    def w_swap(self, part):
        e = self.e
        return self.remote(
            e.SW.at[:, pl.ds(part * e.qd, e.qd)], self.w_ref(self.me, part),
            e.w_send, e.w_recv.at[part, self.z], (2 * self.z + self.c, self.hg),
        )

    def w_take(self, part, zz):
        self.remote_take(self.w_ref(2 * zz + self.c, part), self.e.w_recv.at[part, zz])

    def w_beside(self, part, k):
        for zz in sides(self.z, k):
            self.remote_take(self.units(1), self.e.w_recv.at[part, LINE + zz])

    def units(self, n):
        return self.e.WO.at[pl.ds(0, n * self.e.deep)]

    def remote_take(self, ref, recv):
        self.remote(ref, ref, self.e.w_send, recv, self.partner).wait_recv()

    def remote_left(self, ref, send):
        self.remote(ref, ref, send, self.e.w_recv.at[0, 0], self.partner).wait_send()

    def k_copy(self, zz, way):
        e = self.e
        b = 2 * zz + self.c
        where = ((self.me + 2, self.head), self.partner)[way]
        return self.remote(e.KV.at[b], e.KV.at[b], e.k_send, e.k_recv.at[LINE if way else zz], where)

    def k_onward(self, zz):
        up = zz <= self.z < LINE - 1 and self.z - zz < REACH
        return ([self.k_copy(zz, 0)] if up else []) + [self.k_copy(zz, 1)]

    def k_take(self, zz):
        self.remote_take(self.e.KV.at[2 * zz + self.c], self.e.k_recv.at[zz])

    def k_beside(self):
        n = self.z + 1 - max(self.z - REACH, 0)
        self.remote_take(self.e.KV.at[pl.ds(0, n)], self.e.k_recv.at[LINE])

    def t_copy(self, way):
        e = self.e
        where = (
            self.partner,
            (2 * self.z + 1 - self.x, 2 * self.y + self.x),
            (self.me, 2 * (1 - self.y) + self.x),
        )[way]
        return self.remote(e.TOK, e.X.at[0, self.head], e.t_send, e.t_recv.at[self.head], where)

    def t_take(self, h):
        self.remote_take(self.e.X.at[0, h], self.e.t_recv.at[h])

    def t_relay(self):
        e = self.e
        h, where = ((2 * (1 - self.y) + self.x, self.xn), (2 * self.y + self.x, self.yn))[self.kind]
        return h, self.remote(e.X.at[0, h], e.X.at[0, h], e.t_send, e.t_recv.at[h], where)

    def r_copy(self, h):
        e = self.e
        return self.remote(e.X.at[0, h], e.X.at[1, h], e.r_send, e.r_recv, self.partner)

    def o_copy(self, way, zz, fx, fy, i):
        e = self.e
        b = 2 * zz + (1 - self.x if fx else self.x)
        h = 2 * (1 - self.y) + self.c if fy else self.head
        if way == "c":
            send, recv, where = e.oc_send, e.o_side.at[zz], self.partner
        else:
            fx, fy, where = {
                "up": (fx, fy, (self.me + 2, self.head)),
                "down": (fx, fy, (self.me - 2, self.head)),
                "x": (1, fy, self.xn),
                "y": (fx, 1, self.yn),
            }[way]
            send, recv = e.o_send, e.o_recv.at[2 * fx + fy, zz, i]
        ref = self.o_ref(b, h, i)
        return self.remote(ref, ref, send, recv, where)

    def o_ref(self, b, h, i):
        e = self.e
        piece = e.deep // PIECES
        at = (h * 2 * LINE + b) * e.deep + i * piece
        return e.WO.at[pl.ds(pl.multiple_of(at, 16), piece)]

    def o_onward(self, zz, i):
        return [
            self.o_copy(way, zz, 0, 0, i)
            for way, told in (("up", zz <= self.z < LINE - 1), ("down", zz >= self.z > 0))
            if told
        ]

    def o_share(self, zz, i):
        return [self.o_copy(way, zz, 0, 0, i) for way in ("x", "y", "c")]

    def o_from_x(self, zz, i):
        turn = [self.o_copy("y", zz, 1, 0, i)] if zz not in OVER_X else []
        return turn + [self.o_copy("c", zz, 1, 0, i)]

    def o_from_y(self, zz, i):
        turn = [self.o_copy("x", zz, 0, 1, i)] if zz in OVER_X else []
        return turn + [self.o_copy("c", zz, 0, 1, i)]

    def o_take(self, zz, fx, fy, i):
        self.remote_take(self.o_ref(0, 0, i), self.e.o_recv.at[2 * fx + fy, zz, i])

    def o_beside(self, zz):
        self.remote_take(self.units(4), self.e.o_side.at[zz])

    def a_copy(self, way):
        e = self.e
        where = (
            self.partner, self.yn, self.xn, (2 * self.z + 1 - self.x, 2 * (1 - self.y) + self.c),
        )[way]
        return self.remote(e.AO, e.ATT.at[self.hg], e.a_send, e.a_recv.at[self.hg], where)

    def a_ways(self):
        return (1, 0) if self.kind == 0 else (2, 3)

    def a_pass(self, h):
        e = self.e
        return self.remote(e.ATT.at[h], e.ATT.at[h], e.a_send, e.a_recv.at[h], self.partner)

    def a_order(self):
        x, y = self.x, self.y
        return (2 * y + x, 2 * (1 - y) + x, 2 * y + 1 - x, 2 * (1 - y) + 1 - x)

    def tell(self, zz):
        e = self.e
        if (self.z, self.kind, zz) in e.loaded:
            return
        e.loaded.add((self.z, self.kind, zz))
        for px in range(2):
            self.remote(
                e.SEG.at[self.me], e.SEG.at[self.me], e.s_send, e.s_recv, (2 * zz + px, self.head)
            ).start()

    def do(self, event):
        z, kind, e = self.z, self.kind, self.e
        event = event.name
        name, k = event[:-1], event[-1]
        begin = lambda copies: [copy.start() for copy in copies]
        if name == "W0":
            part = "qk".index(k)
            for move in e.w_loads[kind][part]:
                move.wait()
            begin(self.w_onward(part, z) if kind == 0 else [self.w_swap(part)])
        elif name == "S":
            if kind == 1:
                part = "qk".index(k)
                self.w_take(part, z)
                begin(self.w_onward(part, z))
        elif name in ("Wq", "Wk"):
            part = "qk".index(name[1])
            for zz in sides(z, int(k)):
                self.w_take(part, zz)
                self.tell(zz)
                begin(self.w_onward(part, zz))
        elif event in ("Tp", "Tx", "Ty"):
            if (z, kind) not in e.loaded:
                e.loaded.add((z, kind))
                e.l_tok.wait()
            if event != "Tp" or kind == 1:
                self.t_copy("pxy".index(event[1])).start()
        elif event == "TF":
            h, relay = self.t_relay()
            self.t_take(h)
            relay.start()
        elif name == "On":
            for zz in sides(z, int(k)):
                for i in range(PIECES):
                    if zz != z:
                        self.o_take(zz, 0, 0, i)
                        self.tell(zz)
                    elif i == 0:
                        e.l_out.wait()
                    begin(self.o_onward(zz, i))
        elif name == "Sh":
            for zz in sides(z, int(k)):
                for i in range(PIECES):
                    begin(self.o_share(zz, i))
        elif name in ("Ox", "Oy", "Od"):
            fx, fy = {"x": (1, 0), "y": (0, 1), "d": (1, 1)}[name[1]]
            for zz in sides(z, int(k)):
                for i in range(PIECES):
                    self.o_take(zz, fx, fy, i)
                    if fx and fy:
                        self.o_copy("c", zz, 1, 1, i).start()
                    else:
                        begin(self.o_from_x(zz, i) if fx else self.o_from_y(zz, i))
        elif event == "Kp":
            self.k_beside()
        elif name == "K":
            for zz in sides(z, int(k), False):
                self.k_take(zz)
                begin(self.k_onward(zz))
        else:
            raise ValueError(event)

    def tokens(self):
        e = self.e
        x, y = self.x, self.y
        if self.kind == 0:
            e.l_own.wait()
            self.t_take(2 * y + 1 - x)
            self.t_take(2 * (1 - y) + 1 - x)
            for h in range(4):
                self.r_copy(h).start()
        else:
            self.t_take(2 * y + 1 - x)
            self.t_take(2 * (1 - y))
            self.t_take(2 * (1 - y) + 1)

    def attended(self):
        for way in self.a_ways():
            self.a_copy(way).start()

    def gathered(self, i):
        e = self.e
        h = self.a_order()[i]
        if self.kind == 1 or i > 0:
            self.remote_take(e.ATT.at[h], e.a_recv.at[h])
        if self.kind == 0 and i > 0:
            self.a_pass(h).start()
        if self.kind == 1 and i == 3:
            self.remote_take(e.X.at[1], e.r_recv)

    def emitted(self, k):
        for zz in sides(self.z, k):
            self.o_beside(zz)

    def drain(self):
        z, kind, e = self.z, self.kind, self.e
        onward = 1 if z in (0, LINE - 1) else LINE + 1
        self.remote_left(self.units(2 * (onward + LINE + kind)), e.w_send)
        self.remote_left(self.units(onward + 3 * LINE), e.o_send)
        self.remote_left(self.units(4 * LINE), e.oc_send)
        held = z + 1 - max(z - REACH, 0)
        keys = held + (min(z + 1, REACH) if z < LINE - 1 else 0)
        self.remote_left(e.KV.at[pl.ds(0, keys)], e.k_send)
        self.remote_left(e.X.at[0, pl.ds(0, 3 + kind)], e.t_send)
        self.remote_left(e.KV.at[pl.ds(0, 2 if kind else 5)], e.a_send)
        if kind == 0:
            self.remote_left(e.X.at[0], e.r_send)


class Names:
    pass


def kernel(
    seq, heads, rows, width, most,
    tok, seg_row, wq, wk, wv, wo_in, pre_in, post_in, freq_in,
    out,
    TOK, X, XN, SW, W, WO, SEG, KV, AO, ATT, PR, ACC, RQ, NUM, DEN, pre1, post1, pre, post, freq,
    loc, t_recv, t_send, r_recv, r_send, s_recv, s_send, w_recv, w_send,
    o_recv, o_side, o_send, oc_send, k_recv, k_send, a_recv, a_send,
):
    me, head = lax.axis_index("seq"), lax.axis_index("head")
    z, x = me // 2, lax.rem(me, 2)
    y, c = head // 2, lax.rem(head, 2)
    deep = width // seq
    cut = width // heads
    qd, kd = wq.shape[1], wk.shape[1]
    same = c == x
    other = c != x
    rb = 2 * z + c
    hg = 2 * y + x

    e = Names()
    e.x, e.y, e.deep, e.qd = x, y, deep, qd
    e.loaded = set()
    e.TOK, e.X, e.SW, e.W, e.WO, e.KV, e.AO, e.ATT = TOK, X, SW, W, WO, KV, AO, ATT
    e.t_recv, e.t_send, e.r_recv, e.r_send = t_recv, t_send, r_recv, r_send
    e.w_recv, e.w_send, e.o_recv, e.o_side = w_recv, w_send, o_recv, o_side
    e.o_send, e.oc_send, e.SEG, e.s_recv, e.s_send = o_send, oc_send, SEG, s_recv, s_send
    e.k_recv, e.k_send, e.a_recv, e.a_send = k_recv, k_send, a_recv, a_send

    def load_weights(block):
        return (
            [pltpu.make_async_copy(wq, block.at[:, pl.ds(0, qd)], loc.at[4])],
            [
                pltpu.make_async_copy(wk, block.at[:, pl.ds(qd, kd)], loc.at[5]),
                pltpu.make_async_copy(wv, block.at[:, pl.ds(qd + kd, kd)], loc.at[6]),
            ],
        )

    mine = pl.ds(pl.multiple_of(me * deep, 16), deep)
    e.w_loads = (load_weights(W.at[mine]), load_weights(SW))
    e.l_tok = pltpu.make_async_copy(tok, TOK, loc.at[0])
    e.l_own = pltpu.make_async_copy(tok, X.at[0, head], loc.at[1])
    l_seg = pltpu.make_async_copy(seg_row, SEG.at[me], loc.at[2])
    place = pl.ds(pl.multiple_of((head * seq + me) * deep, 16), deep)
    e.l_out = pltpu.make_async_copy(wo_in, WO.at[place], loc.at[3])
    small = [
        pltpu.make_async_copy(pre_in, pre1, loc.at[7]),
        pltpu.make_async_copy(post_in, post1, loc.at[8]),
        pltpu.make_async_copy(freq_in, freq, loc.at[9]),
    ]

    for kind, told in enumerate((same, other)):
        @pl.when(told)
        def _():
            for part in (1, 0):
                for move in e.w_loads[kind][part]:
                    move.start()

    l_seg.start()
    e.l_tok.start()
    e.l_out.start()

    @pl.when(same)
    def _():
        e.l_own.start()

    for move in small:
        move.start()

    barrier = pltpu.get_barrier_semaphore()

    def greet(where):
        pl.semaphore_signal(barrier, inc=1, device_id=where, device_id_type=MESH)

    for dx in range(2):
        for dy in range(2):
            for dc in range(2):
                if dx + dy + dc > 0:
                    gx = lax.rem(x + dx, 2)
                    greet((2 * z + gx, 2 * lax.rem(y + dy, 2) + lax.rem(c + dc, 2)))

    @pl.when(z > 0)
    def _():
        greet((me - 2, head))

    @pl.when(z < LINE - 1)
    def _():
        greet((me + 2, head))

    ends = (z > 0).astype(jnp.int32) + (z < LINE - 1).astype(jnp.int32)
    pl.semaphore_wait(barrier, 7 + ends)

    l_seg.wait()

    def s_all():
        ref = SEG.at[pl.ds(0, seq - 1)]
        return pltpu.make_async_remote_copy(
            src_ref=ref, dst_ref=ref, send_sem=s_send, recv_sem=s_recv,
            device_id=(lax.rem(me + 1, seq), head), device_id_type=MESH,
        )

    pltpu.make_async_remote_copy(
        src_ref=SEG.at[me], dst_ref=SEG.at[me], send_sem=s_send, recv_sem=s_recv,
        device_id=(2 * z + 1 - x, head), device_id_type=MESH,
    ).start()

    def everyone(act):
        for place in range(LINE):
            for kind, told in enumerate((same, other)):
                @pl.when((z == place) & told)
                def _():
                    act(Moves(place, kind, e))

    def around(k, act):
        if k == 0:
            act(z)
        else:

            @pl.when(z >= k)
            def _():
                act(z - k)

            @pl.when(z + k < LINE)
            def _():
                act(z + k)

    def events(phase):
        def act(moves):
            for event in PLAN[moves.z, moves.kind][phase]:
                moves.do(event)

        everyone(act)

    events(0)
    for move in small:
        move.wait()
    for h in range(heads):
        at = slice(h * cut, (h + 1) * cut)
        pre[0:1, at] = pre1[at][None, :]
        post[0:1, at] = post1[at][None, :]
    everyone(lambda moves: moves.tokens())
    half = rows // 2

    def norm_rows(r, _):
        at = pl.ds(pl.multiple_of(r * half, half), half)
        total = jnp.zeros((half, 1), F32)
        for h in range(heads):
            wide = X[0, h, at, :].astype(F32)
            total += jnp.sum(wide * wide, axis=1, keepdims=True)
        scale = lax.rsqrt(total / width + EPS)
        for h in range(heads):
            gain = pre[0:1, h * cut : (h + 1) * cut]
            XN[h, at, :] = (X[0, h, at, :].astype(F32) * scale * gain).astype(BF16)
        return 0

    lax.fori_loop(0, 2, norm_rows, 0)

    events(1)
    s_all().wait_recv()
    own = jnp.broadcast_to(SEG[rb].astype(F32), (HD, rows))
    col = jnp.transpose(own)[:, 0:1]
    start = jnp.zeros((rows, 1), F32)
    for j in range(seq):
        start += jnp.sum((SEG[j].astype(F32) < col).astype(F32), axis=1, keepdims=True)
    index = (rb * rows + lax.broadcasted_iota(jnp.int32, (rows, 1), 0)).astype(F32)
    angle = (index - start) * freq[...]
    cosine = jnp.cos(angle)
    sine = jnp.sin(angle)
    lane = lax.broadcasted_iota(jnp.int32, (rows, HD), 1)
    sine = jnp.where(lane < HD // 2, -sine, sine)

    def project(part, k):
        cols = slice(part * qd, (part + 1) * qd)
        everyone(lambda moves: moves.w_beside(part, k))

        def add(n):
            some = pl.ds(pl.multiple_of(n * cut, 128), cut)
            value = jnp.dot(XN[n], W[some, cols], preferred_element_type=F32)
            ACC[:, cols] = value if k == 0 else ACC[:, cols] + value

        around(k, add)

    def turn(values):
        return values * cosine + pltpu.roll(values, HD // 2, 1) * sine

    for k in range(LINE):
        events(2 + k)
        project(1, k)
    KV[rb, :, 0:HD] = turn(ACC[:, qd : qd + HD]).astype(BF16)
    KV[rb, :, HD : 2 * HD] = ACC[:, qd + kd : qd + kd + HD].astype(BF16)
    everyone(lambda moves: [copy.start() for copy in moves.k_onward(moves.z)])
    for k in range(LINE):
        events(2 + LINE + k)
        project(0, k)
    for g in range(GROUP):
        RQ[g * rows : (g + 1) * rows, :] = (
            turn(ACC[:, g * HD : (g + 1) * HD]) * SCALAR ** (-0.5)
        ).astype(BF16)

    events(2 + 2 * LINE)
    start2 = jnp.concatenate([start] * GROUP, axis=0)
    index2 = jnp.concatenate([index] * GROUP, axis=0)
    NUM[...] = jnp.zeros_like(NUM)
    DEN[...] = jnp.zeros_like(DEN)

    def attend(j, _):
        s = lax.dot_general(
            RQ[...], KV[j, :, 0:HD], (((1,), (1,)), ((), ())), preferred_element_type=F32
        )
        at = (j * rows + lax.broadcasted_iota(jnp.int32, (1, rows), 1)).astype(F32)
        p = jnp.where(
            (at >= start2) & (at <= index2), jnp.exp(CAP * jnp.tanh(s * (1.0 / CAP))), 0.0
        )
        DEN[...] += jnp.sum(p, axis=1, keepdims=True)
        NUM[...] += jnp.dot(p.astype(BF16), KV[j, :, HD : 2 * HD], preferred_element_type=F32)
        return 0

    lax.fori_loop(jnp.maximum(rb - most // rows, 0), rb + 1, attend, 0)
    ratio = (NUM[...] / DEN[:, 0:1]).astype(BF16)
    for g in range(GROUP):
        AO[:, g * HD : (g + 1) * HD] = ratio[g * rows : (g + 1) * rows, :]
    everyone(lambda moves: moves.attended())

    @pl.when(same)
    def _():
        for g in range(GROUP):
            ATT[hg, :, g * HD : (g + 1) * HD] = ratio[g * rows : (g + 1) * rows, :]

    def emit(i, n):
        acc = lax.dot_general(
            ATT[order[i]], WO[pl.ds(pl.multiple_of(order[i] * width + n * cut, 128), cut), :],
            (((1,), (1,)), ((), ())), preferred_element_type=F32,
        )
        PR[n] = acc if i == 0 else PR[n] + acc

    order = (hg, 2 * (1 - y) + x, 2 * y + 1 - x, 2 * (1 - y) + 1 - x)
    for i in range(heads):
        events(3 + 2 * LINE + i)
        everyone(lambda moves: moves.gathered(i))
        for k in range(LINE - 1):
            if i == 0:
                everyone(lambda moves: moves.emitted(k))
            around(k, functools.partial(emit, i))
    events(3 + 2 * LINE + heads)
    everyone(lambda moves: moves.emitted(LINE - 1))

    def emit_all(n):
        for i in range(heads):
            emit(i, n)

    around(LINE - 1, emit_all)
    squares = jnp.zeros((rows, 1), F32)
    for h in range(heads):
        squares += jnp.sum(PR[h] * PR[h], axis=1, keepdims=True)
    scale = lax.rsqrt(squares / width + EPS)
    kept = other.astype(jnp.int32)

    def finish(h, _):
        at = pl.ds(pl.multiple_of(h * cut, 128), cut)
        out[:, at] = (X[kept, h].astype(F32) + PR[h] * scale * post[0:1, at]).astype(BF16)
        return 0

    lax.fori_loop(0, heads, finish, 0)
    everyone(lambda moves: moves.drain())
    s_all().wait_send()


def fused(tokens, segments, pre_gain, post_gain, w_query, w_key, w_value, w_out):
    seq, heads = lax.axis_size("seq"), lax.axis_size("head")
    rows, cut = tokens.shape
    width = cut * heads
    deep = width // seq
    qd, kd = w_query.shape[1], w_key.shape[1]
    most = rows * seq // 2
    half = HD // 2
    freq = np.float32(10000.0) ** (-(np.arange(half, dtype=np.float32) / np.float32(half)))
    freq = np.concatenate([freq, freq])[None, :].astype(np.float32)
    hbm = pl.BlockSpec(memory_space=pl.ANY)
    vmem = pl.BlockSpec(memory_space=pltpu.VMEM)
    dma = pltpu.SemaphoreType.DMA
    return pl.pallas_call(
        functools.partial(kernel, seq, heads, rows, width, most),
        out_shape=pltpu.VMEM((rows, width), BF16),
        in_specs=[hbm] * 9,
        out_specs=vmem,
        scratch_shapes=[
            pltpu.VMEM((rows, cut), BF16),
            pltpu.VMEM((2, heads, rows, cut), BF16),
            pltpu.VMEM((heads, rows, cut), BF16),
            pltpu.VMEM((deep, qd + 2 * kd), BF16),
            pltpu.VMEM((width, qd + 2 * kd), BF16),
            pltpu.VMEM((heads * width, w_out.shape[0]), BF16),
            pltpu.VMEM((seq, 1, rows), jnp.int32),
            pltpu.VMEM((seq, rows, 2 * HD), BF16),
            pltpu.VMEM((rows, GROUP * HD), BF16),
            pltpu.VMEM((heads, rows, GROUP * HD), BF16),
            pltpu.VMEM((heads, rows, cut), F32),
            pltpu.VMEM((rows, qd + 2 * kd), F32),
            pltpu.VMEM((GROUP * rows, HD), BF16),
            pltpu.VMEM((GROUP * rows, HD), F32),
            pltpu.VMEM((GROUP * rows, HD), F32),
            pltpu.VMEM((width,), F32),
            pltpu.VMEM((width,), F32),
            pltpu.VMEM((1, width), F32),
            pltpu.VMEM((1, width), F32),
            pltpu.VMEM((1, HD), F32),
            dma((10,)),
            dma((heads,)), dma, dma, dma, dma, dma,
            dma((2, 2 * LINE)), dma,
            dma((4, LINE, PIECES)), dma((LINE,)), dma, dma,
            dma((LINE + 1,)), dma, dma((heads,)), dma,
        ],
        compiler_params=pltpu.CompilerParams(
            collective_id=0, has_side_effects=True, vmem_limit_bytes=52 * 2**20
        ),
    )(
        tokens, segments[None, :], w_query, w_key, w_value, w_out.T,
        pre_gain, post_gain, freq,
    )


def solution(mesh):
    specs = (
        P("seq", "head"),
        P("seq"),
        P(),
        P(),
        P("seq", "head"),
        P("seq", "head"),
        P("seq", "head"),
        P("head", "seq"),
    )

    def run(*args):
        small = fits(mesh, args[0].shape, args[5].shape, args[7].shape)
        return jax.shard_map(
            fused if small else local,
            mesh=mesh,
            in_specs=specs,
            out_specs=P("seq", None),
            check_vma=False,
        )(*args)

    return run
```

```python
import enum
import functools

import jax
import jax.numpy as jnp
import numpy as np
from jax import lax
from jax.experimental import pallas as pl
from jax.experimental.pallas import tpu as pltpu
from jax.sharding import PartitionSpec as P

HD = 128
GROUP = 2
SCALAR = 144
DOCS = 8


EPS = 1e-06
CAP = 50.0


def carried_in(value, axis, join, neutral):
    count, mine = (lax.axis_size(axis), lax.axis_index(axis))
    pieces = lax.all_gather(value, axis)
    subtotal = jnp.full_like(value, 0) + jnp.asarray(neutral, value.dtype)

    def step(position, subtotal):
        longer = join(subtotal, pieces[position])
        return jnp.where(position < mine, longer, subtotal)

    return lax.fori_loop(0, count - 1, step, subtotal)


def rotate(values, position, width):
    count = values.shape[1] // width
    half = width // 2
    shaped = values.reshape(values.shape[0], count, width)
    freq = 10000.0 ** (-(jnp.arange(half, dtype=jnp.float32) / half))
    angle = position[:, None] * freq[None, :]
    cosine = jnp.cos(angle)[:, None, :]
    sine = jnp.sin(angle)[:, None, :]
    first = shaped[:, :, :half]
    second = shaped[:, :, half:]
    turned = jnp.concatenate(
        [first * cosine - second * sine, second * cosine + first * sine], axis=2
    )
    return turned.reshape(values.shape[0], count * width)


def add_counts(earlier, later):
    return earlier + later


def local(tokens, segments, pre_gain, post_gain, w_query, w_key, w_value, w_out):
    rows = tokens.shape[0]
    whole = lax.all_gather(tokens, "head", axis=1, tiled=True)
    wide = whole.astype(jnp.float32)
    normed = (
        wide * lax.rsqrt(jnp.mean(wide * wide, axis=1, keepdims=True) + EPS) * pre_gain
    ).astype(jnp.bfloat16)
    pieces = (
        lax.all_gather(w_query, "seq", axis=0, tiled=True),
        lax.all_gather(w_key, "seq", axis=0, tiled=True),
        lax.all_gather(w_value, "seq", axis=0, tiled=True),
    )
    query, key_proj, value_proj = tuple(
        (jnp.dot(normed, piece, preferred_element_type=jnp.float32) for piece in pieces)
    )
    levels = jnp.arange(DOCS, dtype=jnp.int32)
    below = jnp.sum((levels[None, :] > segments[:, None]).astype(jnp.float32), axis=0)
    earlier = carried_in(below, "seq", add_counts, jnp.zeros((DOCS,), jnp.float32))
    starts = earlier + below
    onehot = (segments[:, None] == levels[None, :]).astype(jnp.float32)
    tok_start = jnp.sum(onehot * starts[None, :], axis=1)
    offset = lax.axis_index("seq") * rows
    index_f = (offset + jnp.arange(rows, dtype=jnp.int32)).astype(jnp.float32)
    position = index_f - tok_start
    kv_count = w_key.shape[1] // HD
    rq = (rotate(query, position, HD) * SCALAR ** (-0.5)).astype(jnp.bfloat16)
    rk = rotate(key_proj, position, HD).astype(jnp.bfloat16)
    vb = value_proj.astype(jnp.bfloat16)
    stacked = (
        rq.reshape(rows, kv_count, GROUP, HD)
        .transpose(1, 2, 0, 3)
        .reshape(kv_count, GROUP * rows, HD)
    )
    query_start = jnp.tile(tok_start, GROUP)
    query_index = jnp.tile(index_f, GROUP)
    empty = (
        jnp.zeros((kv_count, GROUP * rows, HD), jnp.float32),
        jnp.zeros((kv_count, GROUP * rows), jnp.float32),
    )
    keys_all = lax.all_gather(rk, "seq", axis=0, tiled=True)
    values_all = lax.all_gather(vb, "seq", axis=0, tiled=True)
    count = keys_all.shape[0]
    block = 1024
    steps_total = count // block

    def compute(offset_blk, state):
        numer, denom = state
        keys_blk = lax.dynamic_slice_in_dim(keys_all, offset_blk, block, 0).reshape(
            block, kv_count, HD
        )
        values_blk = lax.dynamic_slice_in_dim(values_all, offset_blk, block, 0).reshape(
            block, kv_count, HD
        )
        key_index = (offset_blk + jnp.arange(block, dtype=jnp.int32)).astype(jnp.float32)
        scores = jnp.einsum("cqd,kcd->cqk", stacked, keys_blk, preferred_element_type=jnp.float32)
        capped = CAP * jnp.tanh(scores / CAP)
        allowed = (key_index[None, None, :] >= query_start[None, :, None]) & (
            key_index[None, None, :] <= query_index[None, :, None]
        )
        weights = jnp.where(allowed, jnp.exp(capped), 0.0)
        numer = numer + jnp.einsum(
            "cqk,kcd->cqd",
            weights.astype(jnp.bfloat16),
            values_blk,
            preferred_element_type=jnp.float32,
        )
        denom = denom + jnp.sum(weights, axis=2)
        return (numer, denom)

    def one_block(step, state):
        offset_blk = step * block
        return compute(offset_blk, state)

    numer, denom = lax.fori_loop(0, steps_total, one_block, empty)
    attn = (numer / denom[:, :, None]).reshape(kv_count, GROUP, rows, HD).transpose(2, 0, 1, 3)
    attn = attn.reshape(rows, kv_count * GROUP * HD).astype(jnp.bfloat16)
    partial_proj = jnp.dot(
        attn, lax.all_gather(w_out, "seq", axis=1, tiled=True), preferred_element_type=jnp.float32
    )
    partial_proj = lax.optimization_barrier(partial_proj.astype(jnp.bfloat16)).astype(jnp.float32)
    summed = lax.psum(partial_proj.astype(jnp.bfloat16), "head").astype(jnp.float32)
    scale = lax.rsqrt(jnp.mean(summed * summed, axis=1, keepdims=True) + EPS)
    return (wide + summed * scale * post_gain).astype(jnp.bfloat16)


MESH = pl.DeviceIdType.MESH
BF16 = jnp.bfloat16
F32 = jnp.float32
LINE = 4
REACH = LINE // 2
LOG2E = 1.4426950408889634
PIECES = 1
OVER_X = (0,)

class E(enum.Enum):
    K1 = enum.auto()
    K2 = enum.auto()
    Kp = enum.auto()
    Od0 = enum.auto()
    Od1 = enum.auto()
    Od2 = enum.auto()
    Od3 = enum.auto()
    On0 = enum.auto()
    On1 = enum.auto()
    On2 = enum.auto()
    On3 = enum.auto()
    Ox0 = enum.auto()
    Ox1 = enum.auto()
    Ox2 = enum.auto()
    Ox3 = enum.auto()
    Oy0 = enum.auto()
    Oy1 = enum.auto()
    Oy2 = enum.auto()
    Oy3 = enum.auto()
    Sh0 = enum.auto()
    Sh1 = enum.auto()
    Sh2 = enum.auto()
    Sh3 = enum.auto()
    Sk = enum.auto()
    Sq = enum.auto()
    TF = enum.auto()
    Tp = enum.auto()
    Tx = enum.auto()
    Ty = enum.auto()
    W0k = enum.auto()
    W0q = enum.auto()
    Wk1 = enum.auto()
    Wk2 = enum.auto()
    Wk3 = enum.auto()
    Wq1 = enum.auto()
    Wq2 = enum.auto()
    Wq3 = enum.auto()


PLAN = {
    (0, 0): (
        (E.Ty, E.Tp, E.W0q, E.On0, E.W0k, E.Sh0, E.On1, E.Tx, E.On2, E.K2, E.Sk, E.Wk1, E.Sh2, E.TF, E.On3, E.Sh3, E.Sh1, E.Oy3, E.Ox2,),
        (E.Ox0, E.Wk3, E.Ox1, E.Wq1, E.Wk2,),
        (),
        (),
        (),
        (E.Oy2,),
        (E.Wq2, E.Sq, E.Oy0, E.Ox3, E.Wq3, E.K1,),
        (E.Oy1, E.Od1,),
        (),
        (E.Od2,),
        (E.Od0, E.Kp,),
        (),
        (E.Od3,),
        (),
        (),
        (),
    ),
    (0, 1): (
        (E.On0, E.Ty, E.W0k, E.Tx, E.W0q, E.Sk, E.Sh0, E.Tp, E.TF, E.On1, E.Sq, E.On2, E.Wq1, E.Wk1, E.Sh1, E.Sh2,),
        (E.Wk2, E.Ox2,),
        (E.Wk3,),
        (E.Oy2, E.Ox3, E.On3, E.Wq2, E.Sh3, E.Oy0,),
        (E.K2,),
        (),
        (E.Ox1,),
        (E.Od2, E.Wq3, E.Od3,),
        (E.K1, E.Oy3,),
        (),
        (E.Oy1, E.Ox0, E.Od1, E.Kp, E.Od0,),
        (),
        (),
        (),
        (),
        (),
    ),
    (1, 0): (
        (E.Ty, E.Tp, E.On0, E.W0k, E.TF, E.Tx, E.Wk1, E.On1, E.Sh0,),
        (E.Wq3, E.Sk, E.Wk3, E.On2, E.Wq1, E.Sh2, E.W0q, E.Od3, E.Sh1, E.Ox0, E.Wk2, E.Od0, E.On3, E.Ox2,),
        (E.Oy1,),
        (E.K1, E.Sq, E.Oy2, E.Wq2,),
        (),
        (E.Ox1,),
        (E.Oy0,),
        (),
        (E.Od2,),
        (E.K2,),
        (E.Kp, E.Od1, E.Ox3,),
        (),
        (E.Oy3,),
        (),
        (),
        (E.Sh3,),
    ),
    (1, 1): (
        (E.On0, E.Ty, E.W0k, E.W0q, E.Tx, E.Sk, E.Sh0, E.K2, E.Tp, E.On1, E.On3, E.TF, E.Sq, E.Sh1, E.Ox3, E.Wk1,),
        (E.On2, E.Wk3, E.Ox0,),
        (E.Wk2, E.Wq1, E.Sh2,),
        (E.Od0,),
        (),
        (),
        (E.Ox1, E.Oy2, E.Wq2, E.K1, E.Oy3,),
        (E.Kp, E.Oy0, E.Sh3, E.Oy1,),
        (E.Wq3, E.Od1, E.Ox2, E.Od3,),
        (),
        (),
        (E.Od2,),
        (),
        (),
        (),
        (),
    ),
    (2, 0): (
        (E.Ty, E.Tp, E.W0k, E.W0q, E.On0, E.Sk, E.TF, E.Tx, E.Wk3, E.On1, E.Wk1, E.Od3, E.Ox0,),
        (E.Sh0, E.On2, E.Sq, E.Wk2, E.Wq2,),
        (),
        (E.Sh2, E.Sh1,),
        (E.Ox3, E.Ox2, E.Wq1, E.Ox1, E.Oy3, E.K2, E.Oy2, E.Od0, E.Oy0,),
        (E.Oy1,),
        (E.Wq3, E.On3, E.K1, E.Od2, E.Od1,),
        (),
        (E.Sh3,),
        (),
        (E.Kp,),
        (),
        (),
        (),
        (),
        (),
    ),
    (2, 1): (
        (E.Ty, E.On0, E.W0k, E.Sh0, E.W0q, E.On1, E.Tx, E.Sk, E.Tp, E.Sh1, E.Wk1, E.TF, E.Wk2, E.Sq,),
        (E.Od3, E.Ox3, E.On3, E.On2,),
        (E.Sh2,),
        (E.Oy0,),
        (),
        (E.Wq1, E.Wq2, E.Wk3,),
        (),
        (E.Ox1,),
        (),
        (E.K1, E.Wq3, E.Ox2,),
        (E.Sh3, E.Oy1, E.Oy2, E.Ox0, E.K2, E.Kp, E.Od1,),
        (E.Oy3, E.Od0, E.Od2,),
        (),
        (),
        (),
        (),
    ),
    (3, 0): (
        (E.Ty, E.Tp, E.W0q, E.On0, E.W0k, E.On1, E.TF, E.On2, E.Sh0, E.Wk1, E.Wq1, E.Tx, E.Sk, E.Ox2, E.Ox0, E.Sh1, E.On3, E.Ox1, E.Sh2, E.Wk2, E.Od1,),
        (E.Sh3, E.Wq2,),
        (),
        (E.Oy0, E.Sq, E.Wk3,),
        (),
        (E.Od2, E.Oy2,),
        (E.Ox3, E.Oy3,),
        (),
        (E.Wq3,),
        (E.K1, E.K2,),
        (E.Oy1, E.Kp,),
        (E.Od3, E.Od0,),
        (),
        (),
        (),
        (),
    ),
    (3, 1): (
        (E.Ty, E.W0k, E.On0, E.W0q, E.Tx, E.On1, E.Sh0, E.Sk, E.On2, E.Tp, E.TF, E.Sh2, E.Sq,),
        (E.Sh1, E.Wk1, E.Ox0, E.Oy2, E.Wk3, E.On3,),
        (E.Ox2,),
        (E.Wk2, E.Sh3, E.Wq1, E.Od2,),
        (E.Wq2,),
        (E.Oy1, E.K1,),
        (E.Ox1,),
        (E.Ox3, E.Wq3,),
        (),
        (E.K2,),
        (E.Od0, E.Oy3, E.Oy0, E.Kp,),
        (E.Od1,),
        (E.Od3,),
        (),
        (),
        (),
    ),
}


def fits(mesh, tokens, w_key, w_out):
    seq, head = mesh.shape["seq"], mesh.shape["head"]
    width = tokens[1]
    weights = 2 * width * (w_key[1] // head) * (GROUP + 2)
    outs = 2 * w_out[0] * width
    rows = tokens[0] // seq
    rest = rows * width * (4 + 2 + 4 + 2) + tokens[0] * (w_key[1] // head) * 4
    return (
        head == 4
        and seq == 2 * LINE
        and w_key[1] // head == HD
        and (width // head) % 128 == 0
        and (width // seq) % (16 * PIECES) == 0
        and weights + outs + rest < 44 * 2**20
    )


def sides(z, k, down=True):
    return [z] if k == 0 else [at for at in (z - k, z + k if down else -1) if 0 <= at < LINE]


class Moves:
    def __init__(self, z, kind, e):
        self.z, self.kind, self.e = z, kind, e
        x, y = e.x, e.y
        c = x if kind == 0 else 1 - x
        self.x, self.y, self.c = x, y, c
        self.me, self.head = 2 * z + x, 2 * y + c
        self.partner = (self.me, 2 * y + 1 - c)
        self.xn = (2 * z + 1 - x, self.head)
        self.yn = (self.me, 2 * (1 - y) + c)
        self.hg = 2 * y + x

    def remote(self, src, dst, send, recv, where):
        return pltpu.make_async_remote_copy(
            src_ref=src, dst_ref=dst, send_sem=send, recv_sem=recv,
            device_id=where, device_id_type=MESH,
        )

    def w_ref(self, b, part):
        e = self.e
        rows = pl.ds(pl.multiple_of(b * e.deep, 16), e.deep)
        return e.W.at[rows, pl.ds(part * e.qd, e.qd)]

    def w_copy(self, part, zz, way):
        e = self.e
        b = 2 * zz + self.c
        where = ((self.me + 2, self.head), (self.me - 2, self.head), self.partner)[way]
        ref = self.w_ref(b, part)
        return self.remote(ref, ref, e.w_send, e.w_recv.at[part, LINE + zz if way == 2 else zz], where)

    def w_onward(self, part, zz):
        return [
            self.w_copy(part, zz, way)
            for way, told in (
                (0, zz <= self.z < LINE - 1), (1, zz >= self.z > 0), (2, True),
            )
            if told
        ]

    def w_swap(self, part):
        e = self.e
        return self.remote(
            e.SW.at[:, pl.ds(part * e.qd, e.qd)], self.w_ref(self.me, part),
            e.w_send, e.w_recv.at[part, self.z], (2 * self.z + self.c, self.hg),
        )

    def w_take(self, part, zz):
        self.remote_take(self.w_ref(2 * zz + self.c, part), self.e.w_recv.at[part, zz])

    def w_beside(self, part, k):
        for zz in sides(self.z, k):
            self.remote_take(self.units(1), self.e.w_recv.at[part, LINE + zz])

    def units(self, n):
        return self.e.WO.at[pl.ds(0, n * self.e.deep)]

    def remote_take(self, ref, recv):
        self.remote(ref, ref, self.e.w_send, recv, self.partner).wait_recv()

    def remote_left(self, ref, send):
        self.remote(ref, ref, send, self.e.w_recv.at[0, 0], self.partner).wait_send()

    def k_copy(self, zz, way):
        e = self.e
        b = 2 * zz + self.c
        where = ((self.me + 2, self.head), self.partner)[way]
        return self.remote(e.KV.at[b], e.KV.at[b], e.k_send, e.k_recv.at[LINE if way else zz], where)

    def k_onward(self, zz):
        up = zz <= self.z < LINE - 1 and self.z - zz < REACH
        return ([self.k_copy(zz, 0)] if up else []) + [self.k_copy(zz, 1)]

    def k_take(self, zz):
        self.remote_take(self.e.KV.at[2 * zz + self.c], self.e.k_recv.at[zz])

    def k_beside(self):
        n = self.z + 1 - max(self.z - REACH, 0)
        self.remote_take(self.e.KV.at[pl.ds(0, n)], self.e.k_recv.at[LINE])

    def t_copy(self, way):
        e = self.e
        where = (
            self.partner,
            (2 * self.z + 1 - self.x, 2 * self.y + self.x),
            (self.me, 2 * (1 - self.y) + self.x),
        )[way]
        return self.remote(e.TOK, e.X.at[0, self.head], e.t_send, e.t_recv.at[self.head], where)

    def t_take(self, h):
        self.remote_take(self.e.X.at[0, h], self.e.t_recv.at[h])

    def t_relay(self):
        e = self.e
        h, where = ((2 * (1 - self.y) + self.x, self.xn), (2 * self.y + self.x, self.yn))[self.kind]
        return h, self.remote(e.X.at[0, h], e.X.at[0, h], e.t_send, e.t_recv.at[h], where)

    def r_copy(self, h):
        e = self.e
        return self.remote(e.X.at[0, h], e.X.at[1, h], e.r_send, e.r_recv, self.partner)

    def o_copy(self, way, zz, fx, fy, i):
        e = self.e
        b = 2 * zz + (1 - self.x if fx else self.x)
        h = 2 * (1 - self.y) + self.c if fy else self.head
        if way == "c":
            send, recv, where = e.oc_send, e.o_side.at[zz], self.partner
        else:
            fx, fy, where = {
                "up": (fx, fy, (self.me + 2, self.head)),
                "down": (fx, fy, (self.me - 2, self.head)),
                "x": (1, fy, self.xn),
                "y": (fx, 1, self.yn),
            }[way]
            send, recv = e.o_send, e.o_recv.at[2 * fx + fy, zz, i]
        ref = self.o_ref(b, h, i)
        return self.remote(ref, ref, send, recv, where)

    def o_ref(self, b, h, i):
        e = self.e
        piece = e.deep // PIECES
        at = (h * 2 * LINE + b) * e.deep + i * piece
        return e.WO.at[pl.ds(pl.multiple_of(at, 16), piece)]

    def o_onward(self, zz, i):
        return [
            self.o_copy(way, zz, 0, 0, i)
            for way, told in (("up", zz <= self.z < LINE - 1), ("down", zz >= self.z > 0))
            if told
        ]

    def o_share(self, zz, i):
        return [self.o_copy(way, zz, 0, 0, i) for way in ("x", "y", "c")]

    def o_from_x(self, zz, i):
        turn = [self.o_copy("y", zz, 1, 0, i)] if zz not in OVER_X else []
        return turn + [self.o_copy("c", zz, 1, 0, i)]

    def o_from_y(self, zz, i):
        turn = [self.o_copy("x", zz, 0, 1, i)] if zz in OVER_X else []
        return turn + [self.o_copy("c", zz, 0, 1, i)]

    def o_take(self, zz, fx, fy, i):
        self.remote_take(self.o_ref(0, 0, i), self.e.o_recv.at[2 * fx + fy, zz, i])

    def o_beside(self, zz):
        self.remote_take(self.units(4), self.e.o_side.at[zz])

    def a_copy(self, way):
        e = self.e
        where = (
            self.partner, self.yn, self.xn, (2 * self.z + 1 - self.x, 2 * (1 - self.y) + self.c),
        )[way]
        return self.remote(e.AO, e.ATT.at[self.hg], e.a_send, e.a_recv.at[self.hg], where)

    def a_ways(self):
        return (1, 0) if self.kind == 0 else (2, 3)

    def a_pass(self, h):
        e = self.e
        return self.remote(e.ATT.at[h], e.ATT.at[h], e.a_send, e.a_recv.at[h], self.partner)

    def a_order(self):
        x, y = self.x, self.y
        return (2 * y + x, 2 * (1 - y) + x, 2 * y + 1 - x, 2 * (1 - y) + 1 - x)

    def tell(self, zz):
        e = self.e
        if (self.z, self.kind, zz) in e.loaded:
            return
        e.loaded.add((self.z, self.kind, zz))
        for px in range(2):
            self.remote(
                e.SEG.at[self.me], e.SEG.at[self.me], e.s_send, e.s_recv, (2 * zz + px, self.head)
            ).start()

    def do(self, event):
        z, kind, e = self.z, self.kind, self.e
        event = event.name
        name, k = event[:-1], event[-1]
        begin = lambda copies: [copy.start() for copy in copies]
        if name == "W0":
            part = "qk".index(k)
            for move in e.w_loads[kind][part]:
                move.wait()
            begin(self.w_onward(part, z) if kind == 0 else [self.w_swap(part)])
        elif name == "S":
            if kind == 1:
                part = "qk".index(k)
                self.w_take(part, z)
                begin(self.w_onward(part, z))
        elif name in ("Wq", "Wk"):
            part = "qk".index(name[1])
            for zz in sides(z, int(k)):
                self.w_take(part, zz)
                self.tell(zz)
                begin(self.w_onward(part, zz))
        elif event in ("Tp", "Tx", "Ty"):
            if (z, kind) not in e.loaded:
                e.loaded.add((z, kind))
                e.l_tok.wait()
            if event != "Tp" or kind == 1:
                self.t_copy("pxy".index(event[1])).start()
        elif event == "TF":
            h, relay = self.t_relay()
            self.t_take(h)
            relay.start()
        elif name == "On":
            for zz in sides(z, int(k)):
                for i in range(PIECES):
                    if zz != z:
                        self.o_take(zz, 0, 0, i)
                        self.tell(zz)
                    elif i == 0:
                        e.l_out.wait()
                    begin(self.o_onward(zz, i))
        elif name == "Sh":
            for zz in sides(z, int(k)):
                for i in range(PIECES):
                    begin(self.o_share(zz, i))
        elif name in ("Ox", "Oy", "Od"):
            fx, fy = {"x": (1, 0), "y": (0, 1), "d": (1, 1)}[name[1]]
            for zz in sides(z, int(k)):
                for i in range(PIECES):
                    self.o_take(zz, fx, fy, i)
                    if fx and fy:
                        self.o_copy("c", zz, 1, 1, i).start()
                    else:
                        begin(self.o_from_x(zz, i) if fx else self.o_from_y(zz, i))
        elif event == "Kp":
            self.k_beside()
        elif name == "K":
            for zz in sides(z, int(k), False):
                self.k_take(zz)
                begin(self.k_onward(zz))
        else:
            raise ValueError(event)

    def tokens(self):
        e = self.e
        x, y = self.x, self.y
        if self.kind == 0:
            e.l_own.wait()
            self.t_take(2 * y + 1 - x)
            self.t_take(2 * (1 - y) + 1 - x)
            for h in range(4):
                self.r_copy(h).start()
        else:
            self.t_take(2 * y + 1 - x)
            self.t_take(2 * (1 - y))
            self.t_take(2 * (1 - y) + 1)

    def attended(self):
        for way in self.a_ways():
            self.a_copy(way).start()

    def gathered(self, i):
        e = self.e
        h = self.a_order()[i]
        if self.kind == 1 or i > 0:
            self.remote_take(e.ATT.at[h], e.a_recv.at[h])
        if self.kind == 0 and i > 0:
            self.a_pass(h).start()
        if self.kind == 1 and i == 3:
            self.remote_take(e.X.at[1], e.r_recv)

    def emitted(self, k):
        for zz in sides(self.z, k):
            self.o_beside(zz)

    def drain(self):
        z, kind, e = self.z, self.kind, self.e
        onward = 1 if z in (0, LINE - 1) else LINE + 1
        self.remote_left(self.units(2 * (onward + LINE + kind)), e.w_send)
        self.remote_left(self.units(onward + 3 * LINE), e.o_send)
        self.remote_left(self.units(4 * LINE), e.oc_send)
        held = z + 1 - max(z - REACH, 0)
        keys = held + (min(z + 1, REACH) if z < LINE - 1 else 0)
        self.remote_left(e.KV.at[pl.ds(0, keys)], e.k_send)
        self.remote_left(e.X.at[0, pl.ds(0, 3 + kind)], e.t_send)
        self.remote_left(e.KV.at[pl.ds(0, 2 if kind else 5)], e.a_send)
        if kind == 0:
            self.remote_left(e.X.at[0], e.r_send)


class Names:
    pass


def kernel(
    seq, heads, rows, width, most,
    tok, seg_row, wq, wk, wv, wo_in, pre_in, post_in, freq_in,
    out,
    TOK, X, XN, SW, W, WO, SEG, KV, AO, ATT, PR, ACC, RQ, NUM, DEN, pre1, post1, pre, post, freq,
    loc, t_recv, t_send, r_recv, r_send, s_recv, s_send, w_recv, w_send,
    o_recv, o_side, o_send, oc_send, k_recv, k_send, a_recv, a_send,
):
    me, head = lax.axis_index("seq"), lax.axis_index("head")
    z, x = me // 2, lax.rem(me, 2)
    y, c = head // 2, lax.rem(head, 2)
    deep = width // seq
    cut = width // heads
    qd, kd = wq.shape[1], wk.shape[1]
    same = c == x
    other = c != x
    rb = 2 * z + c
    hg = 2 * y + x

    e = Names()
    e.x, e.y, e.deep, e.qd = x, y, deep, qd
    e.loaded = set()
    e.TOK, e.X, e.SW, e.W, e.WO, e.KV, e.AO, e.ATT = TOK, X, SW, W, WO, KV, AO, ATT
    e.t_recv, e.t_send, e.r_recv, e.r_send = t_recv, t_send, r_recv, r_send
    e.w_recv, e.w_send, e.o_recv, e.o_side = w_recv, w_send, o_recv, o_side
    e.o_send, e.oc_send, e.SEG, e.s_recv, e.s_send = o_send, oc_send, SEG, s_recv, s_send
    e.k_recv, e.k_send, e.a_recv, e.a_send = k_recv, k_send, a_recv, a_send

    def load_weights(block):
        return (
            [pltpu.make_async_copy(wq, block.at[:, pl.ds(0, qd)], loc.at[4])],
            [
                pltpu.make_async_copy(wk, block.at[:, pl.ds(qd, kd)], loc.at[5]),
                pltpu.make_async_copy(wv, block.at[:, pl.ds(qd + kd, kd)], loc.at[6]),
            ],
        )

    mine = pl.ds(pl.multiple_of(me * deep, 16), deep)
    e.w_loads = (load_weights(W.at[mine]), load_weights(SW))
    e.l_tok = pltpu.make_async_copy(tok, TOK, loc.at[0])
    e.l_own = pltpu.make_async_copy(tok, X.at[0, head], loc.at[1])
    l_seg = pltpu.make_async_copy(seg_row, SEG.at[me], loc.at[2])
    place = pl.ds(pl.multiple_of((head * seq + me) * deep, 16), deep)
    e.l_out = pltpu.make_async_copy(wo_in, WO.at[place], loc.at[3])
    small = [
        pltpu.make_async_copy(pre_in, pre1, loc.at[7]),
        pltpu.make_async_copy(post_in, post1, loc.at[8]),
        pltpu.make_async_copy(freq_in, freq, loc.at[9]),
    ]

    for kind, told in enumerate((same, other)):
        @pl.when(told)
        def _():
            for part in (1, 0):
                for move in e.w_loads[kind][part]:
                    move.start()

    l_seg.start()
    e.l_tok.start()
    e.l_out.start()

    @pl.when(same)
    def _():
        e.l_own.start()

    for move in small:
        move.start()

    barrier = pltpu.get_barrier_semaphore()

    def greet(where):
        pl.semaphore_signal(barrier, inc=1, device_id=where, device_id_type=MESH)

    for dx in range(2):
        for dy in range(2):
            for dc in range(2):
                if dx + dy + dc > 0:
                    gx = lax.rem(x + dx, 2)
                    greet((2 * z + gx, 2 * lax.rem(y + dy, 2) + lax.rem(c + dc, 2)))

    @pl.when(z > 0)
    def _():
        greet((me - 2, head))

    @pl.when(z < LINE - 1)
    def _():
        greet((me + 2, head))

    ends = (z > 0).astype(jnp.int32) + (z < LINE - 1).astype(jnp.int32)
    pl.semaphore_wait(barrier, 7 + ends)

    l_seg.wait()

    def s_all():
        ref = SEG.at[pl.ds(0, seq - 1)]
        return pltpu.make_async_remote_copy(
            src_ref=ref, dst_ref=ref, send_sem=s_send, recv_sem=s_recv,
            device_id=(lax.rem(me + 1, seq), head), device_id_type=MESH,
        )

    pltpu.make_async_remote_copy(
        src_ref=SEG.at[me], dst_ref=SEG.at[me], send_sem=s_send, recv_sem=s_recv,
        device_id=(2 * z + 1 - x, head), device_id_type=MESH,
    ).start()

    def everyone(act):
        for place in range(LINE):
            for kind, told in enumerate((same, other)):
                @pl.when((z == place) & told)
                def _():
                    act(Moves(place, kind, e))

    def around(k, act):
        if k == 0:
            act(z)
        else:

            @pl.when(z >= k)
            def _():
                act(z - k)

            @pl.when(z + k < LINE)
            def _():
                act(z + k)

    def events(phase):
        def act(moves):
            for event in PLAN[moves.z, moves.kind][phase]:
                moves.do(event)

        everyone(act)

    events(0)
    for move in small:
        move.wait()
    for h in range(heads):
        at = slice(h * cut, (h + 1) * cut)
        pre[0:1, at] = pre1[at][None, :]
        post[0:1, at] = post1[at][None, :]
    everyone(lambda moves: moves.tokens())
    half = rows // 2

    def norm_rows(r, _):
        at = pl.ds(pl.multiple_of(r * half, half), half)
        total = jnp.zeros((half, 1), F32)
        for h in range(heads):
            wide = X[0, h, at, :].astype(F32)
            total += jnp.sum(wide * wide, axis=1, keepdims=True)
        scale = lax.rsqrt(total / width + EPS)
        for h in range(heads):
            gain = pre[0:1, h * cut : (h + 1) * cut]
            XN[h, at, :] = (X[0, h, at, :].astype(F32) * scale * gain).astype(BF16)
        return 0

    lax.fori_loop(0, 2, norm_rows, 0)

    events(1)
    s_all().wait_recv()
    own = jnp.broadcast_to(SEG[rb].astype(F32), (HD, rows))
    col = jnp.transpose(own)[:, 0:1]
    start = jnp.zeros((rows, 1), F32)
    for j in range(seq):
        start += jnp.sum((SEG[j].astype(F32) < col).astype(F32), axis=1, keepdims=True)
    index = (rb * rows + lax.broadcasted_iota(jnp.int32, (rows, 1), 0)).astype(F32)
    angle = (index - start) * freq[...]
    cosine = jnp.cos(angle)
    sine = jnp.sin(angle)
    lane = lax.broadcasted_iota(jnp.int32, (rows, HD), 1)
    sine = jnp.where(lane < HD // 2, -sine, sine)

    def project(part, k):
        cols = slice(part * qd, (part + 1) * qd)
        everyone(lambda moves: moves.w_beside(part, k))

        def add(n):
            some = pl.ds(pl.multiple_of(n * cut, 128), cut)
            value = jnp.dot(XN[n], W[some, cols], preferred_element_type=F32)
            ACC[:, cols] = value if k == 0 else ACC[:, cols] + value

        around(k, add)

    def turn(values):
        return values * cosine + pltpu.roll(values, HD // 2, 1) * sine

    for k in range(LINE):
        events(2 + k)
        project(1, k)
    KV[rb, :, 0:HD] = turn(ACC[:, qd : qd + HD]).astype(BF16)
    KV[rb, :, HD : 2 * HD] = ACC[:, qd + kd : qd + kd + HD].astype(BF16)
    everyone(lambda moves: [copy.start() for copy in moves.k_onward(moves.z)])
    for k in range(LINE):
        events(2 + LINE + k)
        project(0, k)
    for g in range(GROUP):
        RQ[g * rows : (g + 1) * rows, :] = (
            turn(ACC[:, g * HD : (g + 1) * HD]) * SCALAR ** (-0.5)
        ).astype(BF16)

    events(2 + 2 * LINE)
    NUM[...] = jnp.zeros_like(NUM)
    DEN[...] = jnp.zeros_like(DEN)

    start2 = jnp.concatenate([start] * GROUP, axis=0)
    index2 = jnp.concatenate([index] * GROUP, axis=0)

    def attend(j, last):
        s = lax.dot_general(
            RQ[...], KV[j, :, 0:HD], (((1,), (1,)), ((), ())), preferred_element_type=F32
        )
        at = (j * rows + lax.broadcasted_iota(jnp.int32, (1, rows), 1)).astype(F32)
        allowed = at >= start2
        if last:
            allowed = allowed & (at <= index2)
        p = jnp.where(allowed, jnp.exp2((CAP * LOG2E) * jnp.tanh(s * (1.0 / CAP))), 0.0)
        DEN[...] += sum(p[:, k : k + HD] for k in range(0, rows, HD))
        NUM[...] += jnp.dot(p.astype(BF16), KV[j, :, HD : 2 * HD], preferred_element_type=F32)
        return 0

    lax.fori_loop(
        jnp.maximum(rb - most // rows, 0), rb, lambda j, _: attend(j, False), 0
    )
    attend(rb, True)
    ratio = (NUM[...] / jnp.sum(DEN[...], axis=1, keepdims=True)).astype(BF16)
    for g in range(GROUP):
        AO[:, g * HD : (g + 1) * HD] = ratio[g * rows : (g + 1) * rows, :]
    everyone(lambda moves: moves.attended())

    @pl.when(same)
    def _():
        for g in range(GROUP):
            ATT[hg, :, g * HD : (g + 1) * HD] = ratio[g * rows : (g + 1) * rows, :]

    def emit(i, n):
        acc = lax.dot_general(
            ATT[order[i]], WO[pl.ds(pl.multiple_of(order[i] * width + n * cut, 128), cut), :],
            (((1,), (1,)), ((), ())), preferred_element_type=F32,
        )
        PR[n] = acc if i == 0 else PR[n] + acc

    order = (hg, 2 * (1 - y) + x, 2 * y + 1 - x, 2 * (1 - y) + 1 - x)
    for i in range(heads):
        events(3 + 2 * LINE + i)
        everyone(lambda moves: moves.gathered(i))
        for k in range(LINE - 1):
            if i == 0:
                everyone(lambda moves: moves.emitted(k))
            around(k, functools.partial(emit, i))
    events(3 + 2 * LINE + heads)
    everyone(lambda moves: moves.emitted(LINE - 1))

    def emit_all(n):
        for i in range(heads):
            emit(i, n)

    around(LINE - 1, emit_all)
    squares = jnp.zeros((rows, 1), F32)
    for h in range(heads):
        squares += jnp.sum(PR[h] * PR[h], axis=1, keepdims=True)
    scale = lax.rsqrt(squares / width + EPS)
    kept = other.astype(jnp.int32)

    def finish(h, _):
        at = pl.ds(pl.multiple_of(h * cut, 128), cut)
        out[:, at] = (X[kept, h].astype(F32) + PR[h] * scale * post[0:1, at]).astype(BF16)
        return 0

    lax.fori_loop(0, heads, finish, 0)
    everyone(lambda moves: moves.drain())
    s_all().wait_send()


def fused(tokens, segments, pre_gain, post_gain, w_query, w_key, w_value, w_out):
    seq, heads = lax.axis_size("seq"), lax.axis_size("head")
    rows, cut = tokens.shape
    width = cut * heads
    deep = width // seq
    qd, kd = w_query.shape[1], w_key.shape[1]
    most = rows * seq // 2
    half = HD // 2
    freq = np.float32(10000.0) ** (-(np.arange(half, dtype=np.float32) / np.float32(half)))
    freq = np.concatenate([freq, freq])[None, :].astype(np.float32)
    hbm = pl.BlockSpec(memory_space=pl.ANY)
    vmem = pl.BlockSpec(memory_space=pltpu.VMEM)
    dma = pltpu.SemaphoreType.DMA
    return pl.pallas_call(
        functools.partial(kernel, seq, heads, rows, width, most),
        out_shape=pltpu.VMEM((rows, width), BF16),
        in_specs=[hbm] * 9,
        out_specs=vmem,
        scratch_shapes=[
            pltpu.VMEM((rows, cut), BF16),
            pltpu.VMEM((2, heads, rows, cut), BF16),
            pltpu.VMEM((heads, rows, cut), BF16),
            pltpu.VMEM((deep, qd + 2 * kd), BF16),
            pltpu.VMEM((width, qd + 2 * kd), BF16),
            pltpu.VMEM((heads * width, w_out.shape[0]), BF16),
            pltpu.VMEM((seq, 1, rows), jnp.int32),
            pltpu.VMEM((seq, rows, 2 * HD), BF16),
            pltpu.VMEM((rows, GROUP * HD), BF16),
            pltpu.VMEM((heads, rows, GROUP * HD), BF16),
            pltpu.VMEM((heads, rows, cut), F32),
            pltpu.VMEM((rows, qd + 2 * kd), F32),
            pltpu.VMEM((GROUP * rows, HD), BF16),
            pltpu.VMEM((GROUP * rows, HD), F32),
            pltpu.VMEM((GROUP * rows, HD), F32),
            pltpu.VMEM((width,), F32),
            pltpu.VMEM((width,), F32),
            pltpu.VMEM((1, width), F32),
            pltpu.VMEM((1, width), F32),
            pltpu.VMEM((1, HD), F32),
            dma((10,)),
            dma((heads,)), dma, dma, dma, dma, dma,
            dma((2, 2 * LINE)), dma,
            dma((4, LINE, PIECES)), dma((LINE,)), dma, dma,
            dma((LINE + 1,)), dma, dma((heads,)), dma,
        ],
        compiler_params=pltpu.CompilerParams(
            collective_id=0, has_side_effects=True, vmem_limit_bytes=52 * 2**20
        ),
    )(
        tokens, segments[None, :], w_query, w_key, w_value, w_out.T,
        pre_gain, post_gain, freq,
    )


def solution(mesh):
    specs = (
        P("seq", "head"),
        P("seq"),
        P(),
        P(),
        P("seq", "head"),
        P("seq", "head"),
        P("seq", "head"),
        P("head", "seq"),
    )

    def run(*args):
        small = fits(mesh, args[0].shape, args[5].shape, args[7].shape)
        return jax.shard_map(
            fused if small else local,
            mesh=mesh,
            in_specs=specs,
            out_specs=P("seq", None),
            check_vma=False,
        )(*args)

    return run
```

```python
import enum
import functools

import jax
import jax.numpy as jnp
import numpy as np
from jax import lax
from jax.experimental import pallas as pl
from jax.experimental.pallas import tpu as pltpu
from jax.sharding import PartitionSpec as P

HD = 128
GROUP = 2
SCALAR = 144
DOCS = 8


EPS = 1e-06
CAP = 50.0


def carried_in(value, axis, join, neutral):
    count, mine = (lax.axis_size(axis), lax.axis_index(axis))
    pieces = lax.all_gather(value, axis)
    subtotal = jnp.full_like(value, 0) + jnp.asarray(neutral, value.dtype)

    def step(position, subtotal):
        longer = join(subtotal, pieces[position])
        return jnp.where(position < mine, longer, subtotal)

    return lax.fori_loop(0, count - 1, step, subtotal)


def rotate(values, position, width):
    count = values.shape[1] // width
    half = width // 2
    shaped = values.reshape(values.shape[0], count, width)
    freq = 10000.0 ** (-(jnp.arange(half, dtype=jnp.float32) / half))
    angle = position[:, None] * freq[None, :]
    cosine = jnp.cos(angle)[:, None, :]
    sine = jnp.sin(angle)[:, None, :]
    first = shaped[:, :, :half]
    second = shaped[:, :, half:]
    turned = jnp.concatenate(
        [first * cosine - second * sine, second * cosine + first * sine], axis=2
    )
    return turned.reshape(values.shape[0], count * width)


def add_counts(earlier, later):
    return earlier + later


def local(tokens, segments, pre_gain, post_gain, w_query, w_key, w_value, w_out):
    rows = tokens.shape[0]
    whole = lax.all_gather(tokens, "head", axis=1, tiled=True)
    wide = whole.astype(jnp.float32)
    normed = (
        wide * lax.rsqrt(jnp.mean(wide * wide, axis=1, keepdims=True) + EPS) * pre_gain
    ).astype(jnp.bfloat16)
    pieces = (
        lax.all_gather(w_query, "seq", axis=0, tiled=True),
        lax.all_gather(w_key, "seq", axis=0, tiled=True),
        lax.all_gather(w_value, "seq", axis=0, tiled=True),
    )
    query, key_proj, value_proj = tuple(
        (jnp.dot(normed, piece, preferred_element_type=jnp.float32) for piece in pieces)
    )
    levels = jnp.arange(DOCS, dtype=jnp.int32)
    below = jnp.sum((levels[None, :] > segments[:, None]).astype(jnp.float32), axis=0)
    earlier = carried_in(below, "seq", add_counts, jnp.zeros((DOCS,), jnp.float32))
    starts = earlier + below
    onehot = (segments[:, None] == levels[None, :]).astype(jnp.float32)
    tok_start = jnp.sum(onehot * starts[None, :], axis=1)
    offset = lax.axis_index("seq") * rows
    index_f = (offset + jnp.arange(rows, dtype=jnp.int32)).astype(jnp.float32)
    position = index_f - tok_start
    kv_count = w_key.shape[1] // HD
    rq = (rotate(query, position, HD) * SCALAR ** (-0.5)).astype(jnp.bfloat16)
    rk = rotate(key_proj, position, HD).astype(jnp.bfloat16)
    vb = value_proj.astype(jnp.bfloat16)
    stacked = (
        rq.reshape(rows, kv_count, GROUP, HD)
        .transpose(1, 2, 0, 3)
        .reshape(kv_count, GROUP * rows, HD)
    )
    query_start = jnp.tile(tok_start, GROUP)
    query_index = jnp.tile(index_f, GROUP)
    empty = (
        jnp.zeros((kv_count, GROUP * rows, HD), jnp.float32),
        jnp.zeros((kv_count, GROUP * rows), jnp.float32),
    )
    keys_all = lax.all_gather(rk, "seq", axis=0, tiled=True)
    values_all = lax.all_gather(vb, "seq", axis=0, tiled=True)
    count = keys_all.shape[0]
    block = 1024
    steps_total = count // block

    def compute(offset_blk, state):
        numer, denom = state
        keys_blk = lax.dynamic_slice_in_dim(keys_all, offset_blk, block, 0).reshape(
            block, kv_count, HD
        )
        values_blk = lax.dynamic_slice_in_dim(values_all, offset_blk, block, 0).reshape(
            block, kv_count, HD
        )
        key_index = (offset_blk + jnp.arange(block, dtype=jnp.int32)).astype(jnp.float32)
        scores = jnp.einsum("cqd,kcd->cqk", stacked, keys_blk, preferred_element_type=jnp.float32)
        capped = CAP * jnp.tanh(scores / CAP)
        allowed = (key_index[None, None, :] >= query_start[None, :, None]) & (
            key_index[None, None, :] <= query_index[None, :, None]
        )
        weights = jnp.where(allowed, jnp.exp(capped), 0.0)
        numer = numer + jnp.einsum(
            "cqk,kcd->cqd",
            weights.astype(jnp.bfloat16),
            values_blk,
            preferred_element_type=jnp.float32,
        )
        denom = denom + jnp.sum(weights, axis=2)
        return (numer, denom)

    def one_block(step, state):
        offset_blk = step * block
        return compute(offset_blk, state)

    numer, denom = lax.fori_loop(0, steps_total, one_block, empty)
    attn = (numer / denom[:, :, None]).reshape(kv_count, GROUP, rows, HD).transpose(2, 0, 1, 3)
    attn = attn.reshape(rows, kv_count * GROUP * HD).astype(jnp.bfloat16)
    partial_proj = jnp.dot(
        attn, lax.all_gather(w_out, "seq", axis=1, tiled=True), preferred_element_type=jnp.float32
    )
    partial_proj = lax.optimization_barrier(partial_proj.astype(jnp.bfloat16)).astype(jnp.float32)
    summed = lax.psum(partial_proj.astype(jnp.bfloat16), "head").astype(jnp.float32)
    scale = lax.rsqrt(jnp.mean(summed * summed, axis=1, keepdims=True) + EPS)
    return (wide + summed * scale * post_gain).astype(jnp.bfloat16)


MESH = pl.DeviceIdType.MESH
BF16 = jnp.bfloat16
F32 = jnp.float32
LINE = 4
REACH = LINE // 2
LOG2E = 1.4426950408889634
PIECES = 1
OVER_X = (0,)

class E(enum.Enum):
    K1 = enum.auto()
    K2 = enum.auto()
    Kp = enum.auto()
    Od0 = enum.auto()
    Od1 = enum.auto()
    Od2 = enum.auto()
    Od3 = enum.auto()
    On0 = enum.auto()
    On1 = enum.auto()
    On2 = enum.auto()
    On3 = enum.auto()
    Ox0 = enum.auto()
    Ox1 = enum.auto()
    Ox2 = enum.auto()
    Ox3 = enum.auto()
    Oy0 = enum.auto()
    Oy1 = enum.auto()
    Oy2 = enum.auto()
    Oy3 = enum.auto()
    Sh0 = enum.auto()
    Sh1 = enum.auto()
    Sh2 = enum.auto()
    Sh3 = enum.auto()
    Sk = enum.auto()
    Sq = enum.auto()
    TF = enum.auto()
    Tp = enum.auto()
    Tx = enum.auto()
    Ty = enum.auto()
    W0k = enum.auto()
    W0q = enum.auto()
    Wk1 = enum.auto()
    Wk2 = enum.auto()
    Wk3 = enum.auto()
    Wq1 = enum.auto()
    Wq2 = enum.auto()
    Wq3 = enum.auto()


PLAN = {
    (0, 0): (
        (E.On0, E.W0q, E.Sh0, E.W0k, E.Ty, E.On1, E.K2, E.On2, E.Sk, E.Tp, E.Tx, E.Sh2, E.Wk1, E.TF, E.On3, E.Sh3, E.Sh1, E.Ox0,),
        (E.Oy3, E.Ox2, E.Wk3, E.Ox1, E.Wk2,),
        (),
        (E.Wq1,),
        (E.Oy2,),
        (),
        (E.Wq2, E.Sq, E.Oy1, E.Oy0, E.Wq3, E.K1,),
        (E.Od1, E.Ox3,),
        (),
        (),
        (E.Od0, E.Kp,),
        (E.Od2,),
        (E.Od3,),
        (),
        (),
        (),
    ),
    (0, 1): (
        (E.W0k, E.W0q, E.Ty, E.On0, E.Tx, E.Sk, E.Sh0, E.Sq, E.Tp, E.TF, E.On1, E.On2, E.Wq1, E.Wk1, E.Sh2, E.Sh1, E.Wk2,),
        (E.Wk3, E.Ox2, E.Oy2,),
        (E.Ox3,),
        (E.Wq2, E.On3, E.Sh3,),
        (E.Oy0,),
        (),
        (E.Ox1, E.K2, E.Od3, E.Wq3, E.Oy3, E.Oy1,),
        (),
        (E.K1,),
        (),
        (E.Od2, E.Od0, E.Ox0, E.Od1, E.Kp,),
        (),
        (),
        (),
        (),
        (),
    ),
    (1, 0): (
        (E.Wq3, E.Ty, E.W0k, E.On0, E.TF, E.Wk1, E.On1, E.Tp, E.Tx, E.Sh0,),
        (E.Sk, E.Wq1, E.On2, E.W0q, E.Ox0, E.Sh2, E.Sh1, E.Wk3, E.Wk2, E.Od3, E.Ox2,),
        (E.Oy1,),
        (E.On3, E.Od0, E.K1, E.Wq2, E.Sq,),
        (E.Oy2, E.Ox1,),
        (),
        (),
        (E.Oy0,),
        (E.Od2,),
        (E.K2, E.Od1,),
        (E.Kp,),
        (),
        (),
        (E.Oy3,),
        (E.Sh3, E.Ox3,),
        (),
    ),
    (1, 1): (
        (E.K2, E.Ty, E.W0k, E.W0q, E.On0, E.Tx, E.Sk, E.Sh0, E.Tp, E.Sq, E.On1, E.On3, E.TF, E.Sh1, E.Wk3, E.Wk1,),
        (E.Ox3, E.On2, E.Wk2, E.Wq1, E.Ox0,),
        (E.Sh2,),
        (E.Od0,),
        (E.Wq3,),
        (),
        (E.Oy2, E.Ox1, E.Wq2, E.K1, E.Sh3, E.Oy3, E.Oy1,),
        (E.Kp,),
        (E.Oy0,),
        (E.Od3, E.Od1, E.Ox2,),
        (),
        (E.Od2,),
        (),
        (),
        (),
        (),
    ),
    (2, 0): (
        (E.W0k, E.Ty, E.W0q, E.Tp, E.On0, E.TF, E.Tx, E.On1,),
        (E.Sk, E.Ox0, E.Sh0, E.Wk1, E.Od3, E.On2, E.Wk2,),
        (),
        (E.Sq, E.Sh2,),
        (E.Wq1, E.Wq3, E.Sh1, E.Wq2, E.Ox2, E.Oy3, E.Ox1, E.K2, E.Wk3, E.Od0, E.Ox3, E.Oy0, E.Oy2,),
        (E.Oy1,),
        (E.Od2, E.K1, E.On3, E.Sh3,),
        (E.Od1,),
        (),
        (),
        (E.Kp,),
        (),
        (),
        (),
        (),
        (),
    ),
    (2, 1): (
        (E.W0k, E.Ty, E.On0, E.Tp, E.Sh0, E.W0q, E.On1, E.Tx, E.Sh1, E.Sk, E.Wk1, E.TF, E.Wk2, E.Od3, E.Sq,),
        (E.Wq3, E.Ox3, E.Oy0, E.On3,),
        (E.Wk3, E.On2, E.Sh2, E.Wq1,),
        (),
        (E.Wq2,),
        (),
        (),
        (),
        (E.Ox1, E.K1,),
        (E.Oy2, E.Oy1, E.Ox0, E.Ox2, E.Sh3, E.K2, E.Kp,),
        (E.Od1, E.Oy3,),
        (E.Od2, E.Od0,),
        (),
        (),
        (),
        (),
    ),
    (3, 0): (
        (E.W0q, E.Ty, E.TF, E.On0, E.W0k, E.On1, E.Sh0, E.Ox0, E.Tp, E.On2, E.Wq1, E.Wk1, E.Sk, E.Tx, E.Ox2, E.Sh1, E.On3, E.Ox1, E.Wk2, E.Sh2,),
        (E.Od1, E.Sh3,),
        (),
        (E.Wk3, E.Oy0, E.Wq2,),
        (E.Sq, E.Oy2, E.Wq3,),
        (),
        (E.Oy3, E.Ox3, E.Od2,),
        (E.Oy1,),
        (),
        (),
        (E.K1, E.K2, E.Kp,),
        (E.Od3, E.Od0,),
        (),
        (),
        (),
        (),
    ),
    (3, 1): (
        (E.On0, E.W0k, E.W0q, E.Tx, E.Ty, E.Sh0, E.Tp, E.Sk, E.On1, E.Sq, E.On2, E.Sh2, E.TF,),
        (E.Wk3, E.Wk1, E.Sh1, E.Oy2, E.Ox0, E.On3,),
        (E.Ox2, E.Wk2,),
        (E.Sh3,),
        (E.Oy1, E.Wq1,),
        (E.K1, E.Wq3,),
        (E.Wq2,),
        (),
        (),
        (E.K2, E.Ox1, E.Ox3,),
        (E.Oy0, E.Oy3, E.Od0, E.Od2, E.Kp, E.Od3,),
        (E.Od1,),
        (),
        (),
        (),
        (),
    ),
}


def fits(mesh, tokens, w_key, w_out):
    seq, head = mesh.shape["seq"], mesh.shape["head"]
    width = tokens[1]
    weights = 2 * width * (w_key[1] // head) * (GROUP + 2)
    outs = 2 * w_out[0] * width
    rows = tokens[0] // seq
    rest = rows * width * (4 + 2 + 4 + 2) + tokens[0] * (w_key[1] // head) * 4
    return (
        head == 4
        and seq == 2 * LINE
        and w_key[1] // head == HD
        and (width // head) % 128 == 0
        and (width // seq) % (16 * PIECES) == 0
        and weights + outs + rest < 44 * 2**20
    )


def sides(z, k, down=True):
    return [z] if k == 0 else [at for at in (z - k, z + k if down else -1) if 0 <= at < LINE]


class Moves:
    def __init__(self, z, kind, e):
        self.z, self.kind, self.e = z, kind, e
        x, y = e.x, e.y
        c = x if kind == 0 else 1 - x
        self.x, self.y, self.c = x, y, c
        self.me, self.head = 2 * z + x, 2 * y + c
        self.partner = (self.me, 2 * y + 1 - c)
        self.xn = (2 * z + 1 - x, self.head)
        self.yn = (self.me, 2 * (1 - y) + c)
        self.hg = 2 * y + x

    def remote(self, src, dst, send, recv, where):
        return pltpu.make_async_remote_copy(
            src_ref=src, dst_ref=dst, send_sem=send, recv_sem=recv,
            device_id=where, device_id_type=MESH,
        )

    def w_ref(self, b, part):
        e = self.e
        rows = pl.ds(pl.multiple_of(b * e.deep, 16), e.deep)
        return e.W.at[rows, pl.ds(part * e.qd, e.qd)]

    def w_copy(self, part, zz, way):
        e = self.e
        b = 2 * zz + self.c
        where = ((self.me + 2, self.head), (self.me - 2, self.head), self.partner)[way]
        ref = self.w_ref(b, part)
        return self.remote(ref, ref, e.w_send, e.w_recv.at[part, LINE + zz if way == 2 else zz], where)

    def w_onward(self, part, zz):
        return [
            self.w_copy(part, zz, way)
            for way, told in (
                (0, zz <= self.z < LINE - 1), (1, zz >= self.z > 0), (2, True),
            )
            if told
        ]

    def w_swap(self, part):
        e = self.e
        return self.remote(
            e.SW.at[:, pl.ds(part * e.qd, e.qd)], self.w_ref(self.me, part),
            e.w_send, e.w_recv.at[part, self.z], (2 * self.z + self.c, self.hg),
        )

    def w_take(self, part, zz):
        self.remote_take(self.w_ref(2 * zz + self.c, part), self.e.w_recv.at[part, zz])

    def w_beside(self, part, k):
        for zz in sides(self.z, k):
            self.remote_take(self.units(1), self.e.w_recv.at[part, LINE + zz])

    def units(self, n):
        return self.e.WO.at[pl.ds(0, n * self.e.deep)]

    def remote_take(self, ref, recv):
        self.remote(ref, ref, self.e.w_send, recv, self.partner).wait_recv()

    def remote_left(self, ref, send):
        self.remote(ref, ref, send, self.e.w_recv.at[0, 0], self.partner).wait_send()

    def k_copy(self, zz, way):
        e = self.e
        b = 2 * zz + self.c
        where = ((self.me + 2, self.head), self.partner)[way]
        return self.remote(e.KV.at[b], e.KV.at[b], e.k_send, e.k_recv.at[LINE if way else zz], where)

    def k_onward(self, zz):
        up = zz <= self.z < LINE - 1 and self.z - zz < REACH
        return ([self.k_copy(zz, 0)] if up else []) + [self.k_copy(zz, 1)]

    def k_take(self, zz):
        self.remote_take(self.e.KV.at[2 * zz + self.c], self.e.k_recv.at[zz])

    def k_beside(self):
        n = self.z + 1 - max(self.z - REACH, 0)
        self.remote_take(self.e.KV.at[pl.ds(0, n)], self.e.k_recv.at[LINE])

    def t_copy(self, way):
        e = self.e
        where = (
            self.partner,
            (2 * self.z + 1 - self.x, 2 * self.y + self.x),
            (self.me, 2 * (1 - self.y) + self.x),
        )[way]
        return self.remote(e.TOK, e.X.at[0, self.head], e.t_send, e.t_recv.at[self.head], where)

    def t_take(self, h):
        self.remote_take(self.e.X.at[0, h], self.e.t_recv.at[h])

    def t_relay(self):
        e = self.e
        h, where = ((2 * (1 - self.y) + self.x, self.xn), (2 * self.y + self.x, self.yn))[self.kind]
        return h, self.remote(e.X.at[0, h], e.X.at[0, h], e.t_send, e.t_recv.at[h], where)

    def r_copy(self, h):
        e = self.e
        return self.remote(e.X.at[0, h], e.X.at[1, h], e.r_send, e.r_recv, self.partner)

    def o_copy(self, way, zz, fx, fy, i):
        e = self.e
        b = 2 * zz + (1 - self.x if fx else self.x)
        h = 2 * (1 - self.y) + self.c if fy else self.head
        if way == "c":
            send, recv, where = e.oc_send, e.o_side.at[zz], self.partner
        else:
            fx, fy, where = {
                "up": (fx, fy, (self.me + 2, self.head)),
                "down": (fx, fy, (self.me - 2, self.head)),
                "x": (1, fy, self.xn),
                "y": (fx, 1, self.yn),
            }[way]
            send, recv = e.o_send, e.o_recv.at[2 * fx + fy, zz, i]
        ref = self.o_ref(b, h, i)
        return self.remote(ref, ref, send, recv, where)

    def o_ref(self, b, h, i):
        e = self.e
        piece = e.deep // PIECES
        at = (h * 2 * LINE + b) * e.deep + i * piece
        return e.WO.at[pl.ds(pl.multiple_of(at, 16), piece)]

    def o_onward(self, zz, i):
        return [
            self.o_copy(way, zz, 0, 0, i)
            for way, told in (("up", zz <= self.z < LINE - 1), ("down", zz >= self.z > 0))
            if told
        ]

    def o_share(self, zz, i):
        return [self.o_copy(way, zz, 0, 0, i) for way in ("x", "y", "c")]

    def o_from_x(self, zz, i):
        turn = [self.o_copy("y", zz, 1, 0, i)] if zz not in OVER_X else []
        return turn + [self.o_copy("c", zz, 1, 0, i)]

    def o_from_y(self, zz, i):
        turn = [self.o_copy("x", zz, 0, 1, i)] if zz in OVER_X else []
        return turn + [self.o_copy("c", zz, 0, 1, i)]

    def o_take(self, zz, fx, fy, i):
        self.remote_take(self.o_ref(0, 0, i), self.e.o_recv.at[2 * fx + fy, zz, i])

    def o_beside(self, zz):
        self.remote_take(self.units(4), self.e.o_side.at[zz])

    def a_copy(self, way):
        e = self.e
        where = (
            self.partner, self.yn, self.xn, (2 * self.z + 1 - self.x, 2 * (1 - self.y) + self.c),
        )[way]
        return self.remote(e.AO, e.ATT.at[self.hg], e.a_send, e.a_recv.at[self.hg], where)

    def a_ways(self):
        return (1, 0) if self.kind == 0 else (2, 3)

    def a_pass(self, h):
        e = self.e
        return self.remote(e.ATT.at[h], e.ATT.at[h], e.a_send, e.a_recv.at[h], self.partner)

    def a_order(self):
        x, y = self.x, self.y
        return (2 * y + x, 2 * (1 - y) + x, 2 * y + 1 - x, 2 * (1 - y) + 1 - x)

    def tell(self, zz):
        e = self.e
        if (self.z, self.kind, zz) in e.loaded:
            return
        e.loaded.add((self.z, self.kind, zz))
        for px in range(2):
            self.remote(
                e.SEG.at[self.me], e.SEG.at[self.me], e.s_send, e.s_recv, (2 * zz + px, self.head)
            ).start()

    def do(self, event):
        z, kind, e = self.z, self.kind, self.e
        event = event.name
        name, k = event[:-1], event[-1]
        begin = lambda copies: [copy.start() for copy in copies]
        if name == "W0":
            part = "qk".index(k)
            for move in e.w_loads[kind][part]:
                move.wait()
            begin(self.w_onward(part, z) if kind == 0 else [self.w_swap(part)])
        elif name == "S":
            if kind == 1:
                part = "qk".index(k)
                self.w_take(part, z)
                begin(self.w_onward(part, z))
        elif name in ("Wq", "Wk"):
            part = "qk".index(name[1])
            for zz in sides(z, int(k)):
                self.w_take(part, zz)
                self.tell(zz)
                begin(self.w_onward(part, zz))
        elif event in ("Tp", "Tx", "Ty"):
            if (z, kind) not in e.loaded:
                e.loaded.add((z, kind))
                e.l_tok.wait()
            if event != "Tp" or kind == 1:
                self.t_copy("pxy".index(event[1])).start()
        elif event == "TF":
            h, relay = self.t_relay()
            self.t_take(h)
            relay.start()
        elif name == "On":
            for zz in sides(z, int(k)):
                for i in range(PIECES):
                    if zz != z:
                        self.o_take(zz, 0, 0, i)
                        self.tell(zz)
                    elif i == 0:
                        e.l_out.wait()
                    begin(self.o_onward(zz, i))
        elif name == "Sh":
            for zz in sides(z, int(k)):
                for i in range(PIECES):
                    begin(self.o_share(zz, i))
        elif name in ("Ox", "Oy", "Od"):
            fx, fy = {"x": (1, 0), "y": (0, 1), "d": (1, 1)}[name[1]]
            for zz in sides(z, int(k)):
                for i in range(PIECES):
                    self.o_take(zz, fx, fy, i)
                    if fx and fy:
                        self.o_copy("c", zz, 1, 1, i).start()
                    else:
                        begin(self.o_from_x(zz, i) if fx else self.o_from_y(zz, i))
        elif event == "Kp":
            self.k_beside()
        elif name == "K":
            for zz in sides(z, int(k), False):
                self.k_take(zz)
                begin(self.k_onward(zz))
        else:
            raise ValueError(event)

    def tokens(self):
        e = self.e
        x, y = self.x, self.y
        if self.kind == 0:
            e.l_own.wait()
            self.t_take(2 * y + 1 - x)
            self.t_take(2 * (1 - y) + 1 - x)
            for h in range(4):
                self.r_copy(h).start()
        else:
            self.t_take(2 * y + 1 - x)
            self.t_take(2 * (1 - y))
            self.t_take(2 * (1 - y) + 1)

    def attended(self):
        for way in self.a_ways():
            self.a_copy(way).start()

    def gathered(self, i):
        e = self.e
        h = self.a_order()[i]
        if self.kind == 1 or i > 0:
            self.remote_take(e.ATT.at[h], e.a_recv.at[h])
        if self.kind == 0 and i > 0:
            self.a_pass(h).start()
        if self.kind == 1 and i == 3:
            self.remote_take(e.X.at[1], e.r_recv)

    def emitted(self, k):
        for zz in sides(self.z, k):
            self.o_beside(zz)

    def drain(self):
        z, kind, e = self.z, self.kind, self.e
        onward = 1 if z in (0, LINE - 1) else LINE + 1
        self.remote_left(self.units(2 * (onward + LINE + kind)), e.w_send)
        self.remote_left(self.units(onward + 3 * LINE), e.o_send)
        self.remote_left(self.units(4 * LINE), e.oc_send)
        held = z + 1 - max(z - REACH, 0)
        keys = held + (min(z + 1, REACH) if z < LINE - 1 else 0)
        self.remote_left(e.KV.at[pl.ds(0, keys)], e.k_send)
        self.remote_left(e.X.at[0, pl.ds(0, 3 + kind)], e.t_send)
        self.remote_left(e.KV.at[pl.ds(0, 2 if kind else 5)], e.a_send)
        if kind == 0:
            self.remote_left(e.X.at[0], e.r_send)


class Names:
    pass


def kernel(
    seq, heads, rows, width, most,
    tok, seg_row, wq, wk, wv, wo_in, pre_in, post_in, freq_in,
    out,
    TOK, X, XN, SW, W, WO, SEG, KV, AO, ATT, PR, ACC, RQ, NUM, DEN, pre1, post1, pre, post, freq,
    loc, t_recv, t_send, r_recv, r_send, s_recv, s_send, w_recv, w_send,
    o_recv, o_side, o_send, oc_send, k_recv, k_send, a_recv, a_send,
):
    me, head = lax.axis_index("seq"), lax.axis_index("head")
    z, x = me // 2, lax.rem(me, 2)
    y, c = head // 2, lax.rem(head, 2)
    deep = width // seq
    cut = width // heads
    qd, kd = wq.shape[1], wk.shape[1]
    same = c == x
    other = c != x
    rb = 2 * z + c
    hg = 2 * y + x

    e = Names()
    e.x, e.y, e.deep, e.qd = x, y, deep, qd
    e.loaded = set()
    e.TOK, e.X, e.SW, e.W, e.WO, e.KV, e.AO, e.ATT = TOK, X, SW, W, WO, KV, AO, ATT
    e.t_recv, e.t_send, e.r_recv, e.r_send = t_recv, t_send, r_recv, r_send
    e.w_recv, e.w_send, e.o_recv, e.o_side = w_recv, w_send, o_recv, o_side
    e.o_send, e.oc_send, e.SEG, e.s_recv, e.s_send = o_send, oc_send, SEG, s_recv, s_send
    e.k_recv, e.k_send, e.a_recv, e.a_send = k_recv, k_send, a_recv, a_send

    def load_weights(block):
        return (
            [pltpu.make_async_copy(wq, block.at[:, pl.ds(0, qd)], loc.at[4])],
            [
                pltpu.make_async_copy(wk, block.at[:, pl.ds(qd, kd)], loc.at[5]),
                pltpu.make_async_copy(wv, block.at[:, pl.ds(qd + kd, kd)], loc.at[6]),
            ],
        )

    mine = pl.ds(pl.multiple_of(me * deep, 16), deep)
    e.w_loads = (load_weights(W.at[mine]), load_weights(SW))
    e.l_tok = pltpu.make_async_copy(tok, TOK, loc.at[0])
    e.l_own = pltpu.make_async_copy(tok, X.at[0, head], loc.at[1])
    l_seg = pltpu.make_async_copy(seg_row, SEG.at[me], loc.at[2])
    place = pl.ds(pl.multiple_of((head * seq + me) * deep, 16), deep)
    e.l_out = pltpu.make_async_copy(wo_in, WO.at[place], loc.at[3])
    small = [
        pltpu.make_async_copy(pre_in, pre1, loc.at[7]),
        pltpu.make_async_copy(post_in, post1, loc.at[8]),
        pltpu.make_async_copy(freq_in, freq, loc.at[9]),
    ]

    for kind, told in enumerate((same, other)):
        @pl.when(told)
        def _():
            for part in (1, 0):
                for move in e.w_loads[kind][part]:
                    move.start()

    l_seg.start()
    e.l_tok.start()
    e.l_out.start()

    @pl.when(same)
    def _():
        e.l_own.start()

    for move in small:
        move.start()

    barrier = pltpu.get_barrier_semaphore()

    def greet(where):
        pl.semaphore_signal(barrier, inc=1, device_id=where, device_id_type=MESH)

    for dx in range(2):
        for dy in range(2):
            for dc in range(2):
                if dx + dy + dc > 0:
                    gx = lax.rem(x + dx, 2)
                    greet((2 * z + gx, 2 * lax.rem(y + dy, 2) + lax.rem(c + dc, 2)))

    @pl.when(z > 0)
    def _():
        greet((me - 2, head))

    @pl.when(z < LINE - 1)
    def _():
        greet((me + 2, head))

    ends = (z > 0).astype(jnp.int32) + (z < LINE - 1).astype(jnp.int32)
    pl.semaphore_wait(barrier, 7 + ends)

    l_seg.wait()

    def s_all():
        ref = SEG.at[pl.ds(0, seq - 1)]
        return pltpu.make_async_remote_copy(
            src_ref=ref, dst_ref=ref, send_sem=s_send, recv_sem=s_recv,
            device_id=(lax.rem(me + 1, seq), head), device_id_type=MESH,
        )

    pltpu.make_async_remote_copy(
        src_ref=SEG.at[me], dst_ref=SEG.at[me], send_sem=s_send, recv_sem=s_recv,
        device_id=(2 * z + 1 - x, head), device_id_type=MESH,
    ).start()

    def everyone(act):
        for place in range(LINE):
            for kind, told in enumerate((same, other)):
                @pl.when((z == place) & told)
                def _():
                    act(Moves(place, kind, e))

    def around(k, act):
        if k == 0:
            act(z)
        else:

            @pl.when(z >= k)
            def _():
                act(z - k)

            @pl.when(z + k < LINE)
            def _():
                act(z + k)

    def events(phase):
        def act(moves):
            for event in PLAN[moves.z, moves.kind][phase]:
                moves.do(event)

        everyone(act)

    events(0)
    for move in small:
        move.wait()
    for h in range(heads):
        at = slice(h * cut, (h + 1) * cut)
        pre[0:1, at] = pre1[at][None, :]
        post[0:1, at] = post1[at][None, :]
    everyone(lambda moves: moves.tokens())
    half = rows // 2

    def norm_rows(r, _):
        at = pl.ds(pl.multiple_of(r * half, half), half)
        total = jnp.zeros((half, 1), F32)
        for h in range(heads):
            wide = X[0, h, at, :].astype(F32)
            total += jnp.sum(wide * wide, axis=1, keepdims=True)
        scale = lax.rsqrt(total / width + EPS)
        for h in range(heads):
            gain = pre[0:1, h * cut : (h + 1) * cut]
            XN[h, at, :] = (X[0, h, at, :].astype(F32) * scale * gain).astype(BF16)
        return 0

    lax.fori_loop(0, 2, norm_rows, 0)

    events(1)
    s_all().wait_recv()
    own = jnp.broadcast_to(SEG[rb].astype(F32), (HD, rows))
    col = jnp.transpose(own)[:, 0:1]
    start = jnp.zeros((rows, 1), F32)
    for j in range(seq):
        start += jnp.sum((SEG[j].astype(F32) < col).astype(F32), axis=1, keepdims=True)
    index = (rb * rows + lax.broadcasted_iota(jnp.int32, (rows, 1), 0)).astype(F32)
    angle = (index - start) * freq[...]
    cosine = jnp.cos(angle)
    sine = jnp.sin(angle)
    lane = lax.broadcasted_iota(jnp.int32, (rows, HD), 1)
    sine = jnp.where(lane < HD // 2, -sine, sine)

    def project(part, k):
        cols = slice(part * qd, (part + 1) * qd)
        everyone(lambda moves: moves.w_beside(part, k))

        def add(n):
            some = pl.ds(pl.multiple_of(n * cut, 128), cut)
            value = jnp.dot(XN[n], W[some, cols], preferred_element_type=F32)
            ACC[:, cols] = value if k == 0 else ACC[:, cols] + value

        around(k, add)

    def turn(values):
        return values * cosine + pltpu.roll(values, HD // 2, 1) * sine

    for k in range(LINE):
        events(2 + k)
        project(1, k)
    KV[rb, :, 0:HD] = turn(ACC[:, qd : qd + HD]).astype(BF16)
    KV[rb, :, HD : 2 * HD] = ACC[:, qd + kd : qd + kd + HD].astype(BF16)
    everyone(lambda moves: [copy.start() for copy in moves.k_onward(moves.z)])
    for k in range(LINE):
        events(2 + LINE + k)
        project(0, k)
    for g in range(GROUP):
        RQ[g * rows : (g + 1) * rows, :] = (
            turn(ACC[:, g * HD : (g + 1) * HD]) * SCALAR ** (-0.5)
        ).astype(BF16)

    events(2 + 2 * LINE)
    NUM[...] = jnp.zeros_like(NUM)
    DEN[...] = jnp.zeros_like(DEN)

    start2 = jnp.concatenate([start] * GROUP, axis=0)
    index2 = jnp.concatenate([index] * GROUP, axis=0)

    def attend(j, last):
        s = lax.dot_general(
            RQ[...], KV[j, :, 0:HD], (((1,), (1,)), ((), ())), preferred_element_type=F32
        )
        at = (j * rows + lax.broadcasted_iota(jnp.int32, (1, rows), 1)).astype(F32)
        allowed = at >= start2
        if last:
            allowed = allowed & (at <= index2)
        p = jnp.where(allowed, jnp.exp2((CAP * LOG2E) * jnp.tanh(s * (1.0 / CAP))), 0.0)
        DEN[...] += sum(p[:, k : k + HD] for k in range(0, rows, HD))
        NUM[...] += jnp.dot(p.astype(BF16), KV[j, :, HD : 2 * HD], preferred_element_type=F32)
        return 0

    lax.fori_loop(
        jnp.maximum(rb - most // rows, 0), rb, lambda j, _: attend(j, False), 0
    )
    attend(rb, True)
    ratio = (NUM[...] / jnp.sum(DEN[...], axis=1, keepdims=True)).astype(BF16)
    for g in range(GROUP):
        AO[:, g * HD : (g + 1) * HD] = ratio[g * rows : (g + 1) * rows, :]
    everyone(lambda moves: moves.attended())

    @pl.when(same)
    def _():
        for g in range(GROUP):
            ATT[hg, :, g * HD : (g + 1) * HD] = ratio[g * rows : (g + 1) * rows, :]

    def emit(i, n):
        acc = lax.dot_general(
            ATT[order[i]], WO[pl.ds(pl.multiple_of(order[i] * width + n * cut, 128), cut), :],
            (((1,), (1,)), ((), ())), preferred_element_type=F32,
        )
        value = acc if i == 0 else PR[n] + acc
        PR[n] = value
        if i == heads - 1:
            square = value * value
            DEN[0:rows, :] += sum(square[:, k : k + HD] for k in range(0, cut, HD))

    order = (hg, 2 * (1 - y) + x, 2 * y + 1 - x, 2 * (1 - y) + 1 - x)
    DEN[...] = jnp.zeros_like(DEN)
    for i in range(heads):
        if i == heads - 1:
            events(3 + 2 * LINE + i)
            everyone(lambda moves: moves.emitted(LINE - 1))
            for past in range(i):
                around(LINE - 1, functools.partial(emit, past))
        events(3 + 2 * LINE + i + i // (heads - 1))
        everyone(lambda moves: moves.gathered(i))
        for k in range(LINE - 1 + i // (heads - 1)):
            if i == 0:
                everyone(lambda moves: moves.emitted(k))
            around(k, functools.partial(emit, i))
    squares = jnp.sum(DEN[0:rows, :], axis=1, keepdims=True)
    scale = lax.rsqrt(squares / width + EPS)
    kept = other.astype(jnp.int32)

    def finish(h, _):
        at = pl.ds(pl.multiple_of(h * cut, 128), cut)
        out[:, at] = (X[kept, h].astype(F32) + PR[h] * scale * post[0:1, at]).astype(BF16)
        return 0

    lax.fori_loop(0, heads, finish, 0)
    everyone(lambda moves: moves.drain())
    s_all().wait_send()


def fused(tokens, segments, pre_gain, post_gain, w_query, w_key, w_value, w_out):
    seq, heads = lax.axis_size("seq"), lax.axis_size("head")
    rows, cut = tokens.shape
    width = cut * heads
    deep = width // seq
    qd, kd = w_query.shape[1], w_key.shape[1]
    most = rows * seq // 2
    half = HD // 2
    freq = np.float32(10000.0) ** (-(np.arange(half, dtype=np.float32) / np.float32(half)))
    freq = np.concatenate([freq, freq])[None, :].astype(np.float32)
    hbm = pl.BlockSpec(memory_space=pl.ANY)
    vmem = pl.BlockSpec(memory_space=pltpu.VMEM)
    dma = pltpu.SemaphoreType.DMA
    return pl.pallas_call(
        functools.partial(kernel, seq, heads, rows, width, most),
        out_shape=pltpu.VMEM((rows, width), BF16),
        in_specs=[hbm] * 9,
        out_specs=vmem,
        scratch_shapes=[
            pltpu.VMEM((rows, cut), BF16),
            pltpu.VMEM((2, heads, rows, cut), BF16),
            pltpu.VMEM((heads, rows, cut), BF16),
            pltpu.VMEM((deep, qd + 2 * kd), BF16),
            pltpu.VMEM((width, qd + 2 * kd), BF16),
            pltpu.VMEM((heads * width, w_out.shape[0]), BF16),
            pltpu.VMEM((seq, 1, rows), jnp.int32),
            pltpu.VMEM((seq, rows, 2 * HD), BF16),
            pltpu.VMEM((rows, GROUP * HD), BF16),
            pltpu.VMEM((heads, rows, GROUP * HD), BF16),
            pltpu.VMEM((heads, rows, cut), F32),
            pltpu.VMEM((rows, qd + 2 * kd), F32),
            pltpu.VMEM((GROUP * rows, HD), BF16),
            pltpu.VMEM((GROUP * rows, HD), F32),
            pltpu.VMEM((GROUP * rows, HD), F32),
            pltpu.VMEM((width,), F32),
            pltpu.VMEM((width,), F32),
            pltpu.VMEM((1, width), F32),
            pltpu.VMEM((1, width), F32),
            pltpu.VMEM((1, HD), F32),
            dma((10,)),
            dma((heads,)), dma, dma, dma, dma, dma,
            dma((2, 2 * LINE)), dma,
            dma((4, LINE, PIECES)), dma((LINE,)), dma, dma,
            dma((LINE + 1,)), dma, dma((heads,)), dma,
        ],
        compiler_params=pltpu.CompilerParams(
            collective_id=0, has_side_effects=True, vmem_limit_bytes=52 * 2**20
        ),
    )(
        tokens, segments[None, :], w_query, w_key, w_value, w_out.T,
        pre_gain, post_gain, freq,
    )


def solution(mesh):
    specs = (
        P("seq", "head"),
        P("seq"),
        P(),
        P(),
        P("seq", "head"),
        P("seq", "head"),
        P("seq", "head"),
        P("head", "seq"),
    )

    def run(*args):
        small = fits(mesh, args[0].shape, args[5].shape, args[7].shape)
        return jax.shard_map(
            fused if small else local,
            mesh=mesh,
            in_specs=specs,
            out_specs=P("seq", None),
            check_vma=False,
        )(*args)

    return run
```
